32 devices in a mesh: job: 2 (over y), row: 4 (over z), col: 2 (over x), samp: 2 (over core).
Axes of the slice: x: 2, y: 2, z: 4, core: 2. Of those that a mesh axis runs over, the one named last changes fastest.
Arguments:
- pair_repr: bfloat16 [256, 128, 128], P(('job', 'row'), ('col', 'samp')), parts along dimension 0, may hold values from -100 to 100
- asym_id: int32 [256], P('job'), parts along dimension 0, may hold values from 0 to 7, never falling along the last dimension, each value on 1 to 32 neighbouring positions
- valid_len: int32 [2], P('job'), parts along dimension 0, may hold values from 64 to 128
- rel_embed: bfloat16 [128, 128], replicated, may hold values from -12 to 12
- pair_gain: float32 [128], replicated, may hold values from 0.25 to 1.75
- bias_weight: bfloat16 [128, 16], replicated, may hold values from -64 to 64
- tokens: bfloat16 [32, 128, 768], P(('job', 'col', 'samp'), 'row'), parts along dimension 0, may hold values from -6 to 6
- token_gain: float32 [1, 768], replicated, may hold values from 0.25 to 1.75
- qkv_weight: bfloat16 [1, 3, 768, 768], P(None, None, None, 'row'), may hold values from -0.21875 to 0.21875
- out_weight: bfloat16 [1, 768, 768], P(None, 'row'), may hold values from -0.21875 to 0.21875
Outputs:
- refined: bfloat16 [32, 128, 768], P(('job', 'col', 'samp'), 'row'), parts along dimension 0
The draws below stay inside these ranges and needn't reach their ends.
There are 2 independent parts, one for each index of `job`. The reference program is written for one: setup_inputs(seed, part) draws one part's arguments, and reference() takes and returns one part's arrays. A program takes and returns all parts, laid end to end along the dimension named above; an argument that names none is the same for every part. Nothing has to cross between parts.
Inputs may be any that keep to these rules, and one draw needn't show every extreme that they name: `asym_id`: chain indices never fall along the tokens.
All inputs are finite; a program needn't handle non-finite values.
Results may differ from the reference program's by a relative error of at most 0.002.
The reference program's roundings to bfloat16 on the way count: a program that leaves them out, or rounds other values in their place, can miss the bound.
Values may be sent and summed in bfloat16 or wider, within the bound.
A program may use at most 64 MiB of HBM per device.

```python
import math
import jax
import jax.numpy as jnp
import numpy as np
from jax import lax

PAIR_C = 128
D = 768
HEADS = 16
HEAD_DIM = 48
REL = 128
LAYERS = 1
TOKENS = 128
SAMPLES = 16
N_ROW = 4


def draw_pair_repr(key, part):
    noise_key, scale_key = jax.random.split(key, 2)
    scales = jnp.exp(jax.random.uniform(scale_key, (TOKENS, TOKENS, 1), jnp.float32, 0.0, math.log(10.0)))
    values = jax.random.normal(noise_key, (TOKENS, TOKENS, PAIR_C), jnp.float32) * scales
    return jnp.clip(values, -100.0, 100.0).astype(jnp.bfloat16)


def draw_bias_weight(key, part):
    noise_key = jax.random.fold_in(key, 0)
    strength = jnp.full((1, HEADS), 2.5, jnp.float32)
    spread = strength / math.sqrt(PAIR_C)
    values = jax.random.normal(noise_key, (PAIR_C, HEADS), jnp.float32) * spread
    return jnp.clip(values, -6.0 * spread, 6.0 * spread).astype(jnp.bfloat16)


def level_of(key, dims, cuts, smallest, top_value):
    factor_of, own = 1.0, jax.random.fold_in(key, 6)
    for position, shards_of in cuts:
        draws = jnp.exp(jax.random.uniform(jax.random.fold_in(own, position), (shards_of,), jnp.float32, smallest / len(cuts), top_value / len(cuts)))
        factor_of = factor_of * jnp.repeat(draws, dims[position] // shards_of).reshape([-1 if axis == position else 1 for axis in range(len(dims))])
    return factor_of


def length_profile(amount, total, most, skew):
    weights = [(1 << 20) // math.isqrt(rank ** skew) + 1 for rank in range(2, amount + 1)]
    spare, holding = total - most - (amount - 1), [1] * (amount - 1)
    while spare > 0:
        movable = [i for i in range(amount - 1) if holding[i] < most]
        pool, budget = sum([weights[i] for i in movable]), spare
        for i in movable:
            addition = min(most - holding[i], max(1, budget * weights[i] // pool), spare)
            holding[i] = holding[i] + addition
            spare = spare - addition
    return np.array([most] + holding)


def uneven(own_key, count, total, limit, skew):
    if count == 2:
        one = jax.random.randint(own_key, (), max(1, total - limit), min(limit, total - 1) + 1)
        return jnp.stack([one, total - one])
    sizes = jnp.asarray(length_profile(count, total, limit, skew), jnp.int32)
    couples = (count - 1) // 2
    giver, sink = sizes[1:1 + 2 * couples:2], sizes[2:2 + 2 * couples:2]
    room = jnp.minimum(giver - 1, limit - sink)
    moved = jax.random.randint(jax.random.fold_in(own_key, 1), (couples,), 0, 1 << 20) % (room + 1)
    sizes = sizes.at[1:1 + 2 * couples:2].set(giver - moved).at[2:2 + 2 * couples:2].set(sink + moved)
    return sizes[jax.random.permutation(jax.random.fold_in(own_key, 2), count)]


def normal_values(stream_key, shape, deviation, reach, shards=(), held_as=jnp.bfloat16):
    array = jax.random.normal(stream_key, shape, jnp.float32) * deviation
    if len(shards) > 0:
        array = level_of(stream_key, shape, shards, -0.22, 0.18) * array
    return jnp.clip(array, min=-reach, max=reach).astype(held_as)


def setup_inputs(seed: int = 0, part: int = 0) -> dict:
    arg_keys = jax.random.split(jax.random.key(seed), 11)
    own_keys = jax.random.split(jax.random.fold_in(arg_keys[10], part), 11)
    pair_repr = draw_pair_repr(jax.random.fold_in(jax.random.fold_in(arg_keys[10], part), 71), part)
    asym_id = jnp.searchsorted(jnp.cumsum(uneven(own_keys[1], 8, TOKENS, TOKENS // 4, 1)), jnp.arange(TOKENS), side="right").astype(jnp.int32)
    valid_len = jax.random.randint(own_keys[2], (1,), TOKENS // 2, TOKENS + 1).astype(jnp.int32)
    rel_embed = normal_values(arg_keys[3], (REL, PAIR_C), 2.0, 12.0)
    pair_gain = jnp.clip(1.0 + 0.15 * jax.random.normal(arg_keys[4], (PAIR_C,), jnp.float32), 0.25, 1.75)
    bias_weight = draw_bias_weight(jax.random.fold_in(arg_keys[10], 71), part)
    tokens = normal_values(own_keys[6], (SAMPLES, TOKENS, D), 1.0, 6.0, ((0, 4), (1, 4)))
    token_gain = jnp.clip(1.0 + 0.15 * jax.random.normal(arg_keys[7], (LAYERS, D), jnp.float32), 0.25, 1.75)
    qkv_weight = normal_values(arg_keys[8], (LAYERS, 3, D, D), D ** -0.5, 0.21875, ((3, 4),))
    out_weight = normal_values(arg_keys[9], (LAYERS, D, D), D ** -0.5, 0.21875, ((1, 4),))
    return dict(pair_repr=pair_repr, asym_id=asym_id, valid_len=valid_len, rel_embed=rel_embed, pair_gain=pair_gain, bias_weight=bias_weight, tokens=tokens, token_gain=token_gain, qkv_weight=qkv_weight, out_weight=out_weight)


epsilon = 1e-05

def normalize(values, gain_vector):
    average = lax.optimization_barrier(jnp.mean(values, axis=-1, keepdims=True))
    centered = values - average
    variance = lax.optimization_barrier(jnp.mean(centered * centered, axis=-1, keepdims=True))
    return centered * lax.rsqrt(variance + epsilon) * gain_vector

def attend_sample(queries, key_rows, value_rows, pair_bias, keymask):
    query_f = queries.astype(jnp.float32).reshape(TOKENS, HEADS, HEAD_DIM)
    key_f = key_rows.astype(jnp.float32).reshape(TOKENS, HEADS, HEAD_DIM)
    value_f = value_rows.astype(jnp.float32).reshape(TOKENS, HEADS, HEAD_DIM)
    scores = jnp.einsum('ihd,jhd->hij', query_f, key_f) / math.sqrt(HEAD_DIM) + pair_bias
    scores = jnp.where(keymask[None, None, :], scores, -1e+30)
    row_max = lax.optimization_barrier(jnp.max(scores, axis=-1, keepdims=True))
    weights = jnp.where(keymask[None, None, :], jnp.exp(scores - row_max), 0.0)
    row_total = lax.optimization_barrier(jnp.sum(weights, axis=-1, keepdims=True))
    probs = (weights / row_total).astype(jnp.bfloat16)
    attended = jnp.einsum('hij,jhd->ihd', probs.astype(jnp.float32), value_f)
    return attended.reshape(TOKENS, D).astype(jnp.bfloat16)

def reference(pair_repr, asym_id, valid_len, rel_embed, pair_gain, bias_weight, tokens, token_gain, qkv_weight, out_weight):
    block_rows = TOKENS // N_ROW
    positions = jnp.arange(TOKENS, dtype=jnp.int32)
    reach_max = REL // 2 - 1

    def bias_block(block_index):
        first_row = (block_index * block_rows).astype(jnp.int32)
        pair_rows = lax.dynamic_slice_in_dim(pair_repr, first_row, block_rows, 0)
        row_ids = first_row + jnp.arange(block_rows, dtype=jnp.int32)
        row_chain = lax.dynamic_slice_in_dim(asym_id, first_row, block_rows, 0)
        offset = jnp.clip(row_ids[:, None] - positions[None, :], -reach_max, reach_max) + reach_max
        bin_ids = jnp.where(row_chain[:, None] == asym_id[None, :], offset, REL - 1)
        onehot = (bin_ids.reshape(-1)[:, None] == jnp.arange(REL, dtype=jnp.int32)[None, :]).astype(jnp.bfloat16)
        summed = pair_rows.reshape(-1, PAIR_C).astype(jnp.float32) + jnp.dot(onehot, rel_embed, preferred_element_type=jnp.float32)
        normed = normalize(summed, pair_gain).astype(jnp.bfloat16)
        projected = lax.dot_general(bias_weight, normed, (((0,), (1,)), ((), ())), preferred_element_type=jnp.float32)
        return projected.reshape(HEADS, block_rows, TOKENS)
    blocks = lax.map(bias_block, jnp.arange(N_ROW, dtype=jnp.int32))
    pair_bias = jnp.transpose(blocks, (1, 0, 2, 3)).reshape(HEADS, TOKENS, TOKENS)
    keymask = positions < valid_len[0]
    current = tokens
    for layer_index in range(LAYERS):
        normed_tok = normalize(current.astype(jnp.float32), token_gain[layer_index]).astype(jnp.bfloat16)
        flat = normed_tok.reshape(-1, D)
        parts = []
        for part_index in range(3):
            product = jnp.dot(flat, qkv_weight[layer_index, part_index], preferred_element_type=jnp.float32)
            parts.append(product.astype(jnp.bfloat16).reshape(SAMPLES, TOKENS, D))

        def one_sample(sample_item):
            return attend_sample(sample_item[0], sample_item[1], sample_item[2], pair_bias, keymask)
        attended = lax.map(one_sample, (parts[0], parts[1], parts[2]))
        update = jnp.dot(attended.reshape(-1, D), out_weight[layer_index], preferred_element_type=jnp.float32)
        current = (current.astype(jnp.float32) + update.reshape(SAMPLES, TOKENS, D)).astype(jnp.bfloat16)
    return current
```

```python
import contextlib
import functools
import math

import jax
import jax.numpy as jnp
from jax import lax
from jax.experimental import pallas as pl
from jax.experimental.pallas import tpu as pltpu
from jax.sharding import PartitionSpec as P

HEAD_DIM = 48
EPSILON = 1e-05
LANES = 128
MESH = pl.DeviceIdType.MESH
mark = contextlib.nullcontext


def normalize(values, gain_vector):
    average = jnp.mean(values, axis=-1, keepdims=True)
    centered = values - average
    variance = jnp.mean(centered * centered, axis=-1, keepdims=True)
    return centered * lax.rsqrt(variance + EPSILON) * gain_vector


def back(position, shift, size):
    return lax.rem(position + (size - shift), size) if shift else position


def aligned(value, unit):
    return value if isinstance(value, int) else pl.multiple_of(value, unit)


def kernel(
    axes,
    cuts,
    asym_hbm,
    valid_hbm,
    pair_hbm,
    rel_hbm,
    pair_gain_hbm,
    bias_weight_hbm,
    tokens_hbm,
    token_gain_hbm,
    qkv_hbm,
    out_weight_hbm,
    out,
    asym,
    valid,
    pair,
    rel,
    pair_gain,
    bias_weight,
    token_gain,
    qkv,
    tok,
    ow,
    bias_send,
    bias_recv,
    bias,
    query,
    key,
    value,
    attended,
    heads_in,
    local_sem,
    tok_got,
    tok_sent,
    bias_got,
    ow_got,
    att_got,
    sent,
):
    n_job, n_row, n_col, n_samp = axes
    job, me = lax.axis_index("job"), lax.axis_index("row")
    col, samp = lax.axis_index("col"), lax.axis_index("samp")
    samples, token_rows, width = tokens_hbm.shape
    total = n_row * token_rows
    tile_rows, tile_cols, channels = pair.shape
    bins = rel.shape[0]
    plane = col * n_samp + samp
    all_heads = bias_weight.shape[0]
    local_heads = all_heads // n_row
    local_width = local_heads * HEAD_DIM
    fold = LANES // tile_cols
    stripes = tile_rows // fold
    part_rows = bias_recv.shape[1]
    out_rows = ow.shape[1]
    n_plane = n_col * n_samp
    p_job, p_col, p_samp = cuts
    pieces = p_job * p_col * p_samp
    piece_rows, piece_cols = out_rows // (p_job * p_samp), width // p_col
    here = (job if p_job > 1 else 0, col if p_col > 1 else 0, samp if p_samp > 1 else 0)

    def row_peer(k):
        return lax.rem(me + k, n_row)

    def row_source(k):
        return back(me, k, n_row)

    def send(source, target, left, got, device):
        pltpu.make_async_remote_copy(
            src_ref=source,
            dst_ref=target,
            send_sem=left,
            recv_sem=got,
            device_id=device,
            device_id_type=MESH,
        ).start()

    def awaiting(ref, semaphore):
        return pltpu.make_async_remote_copy(
            src_ref=ref,
            dst_ref=ref,
            send_sem=semaphore,
            recv_sem=semaphore,
            device_id={"row": row_peer(1)},
            device_id_type=MESH,
        )

    def arrive(ref, semaphore):
        awaiting(ref, semaphore).wait_recv()

    barrier = pltpu.get_barrier_semaphore()
    greeted = 0
    for k in range(1, n_row):
        pl.semaphore_signal(barrier, inc=1, device_id={"row": row_peer(k)}, device_id_type=MESH)
        greeted += 1
    for a in range(p_job):
        for b in range(n_col):
            for c in range(n_samp):
                device = {
                    name: lax.rem(spot + step, size)
                    for name, spot, step, size in zip(
                        ("job", "col", "samp"), (job, col, samp), (a, b, c), (n_job, n_col, n_samp)
                    )
                    if step
                }
                if device:
                    pl.semaphore_signal(barrier, inc=1, device_id=device, device_id_type=MESH)
                    greeted += 1

    loads = {}
    for index, (name, source, target) in enumerate(
        (
            ("asym", asym_hbm, asym),
            ("pair", pair_hbm, pair),
            ("rel", rel_hbm, rel),
            ("pair_gain", pair_gain_hbm, pair_gain),
            ("bias_weight", bias_weight_hbm, bias_weight),
            ("qkv", qkv_hbm.at[0], qkv),
            ("token_gain", token_gain_hbm, token_gain),
            ("ow", out_weight_hbm.at[0], ow.at[me]),
            ("valid", valid_hbm, valid),
        )
    ):
        loads[name] = pltpu.make_async_copy(source, target, local_sem.at[index])
    loads["tok"] = pltpu.make_async_copy(tokens_hbm, tok.at[:, me], local_sem.at[9])
    for name in ("asym", "pair", "rel", "pair_gain", "bias_weight", "tok", "qkv", "token_gain", "ow", "valid"):
        loads[name].start()

    with mark("pairload"):
        for name in ("asym", "pair", "rel", "pair_gain", "bias_weight"):
            loads[name].wait()
    first_row, first_col = me * tile_rows, plane * tile_cols
    sub = lax.broadcasted_iota(jnp.int32, (tile_cols, LANES), 0)
    lane = lax.broadcasted_iota(jnp.int32, (tile_cols, LANES), 1)
    with mark("pair"):
        col_chain = jnp.zeros((tile_cols, LANES), jnp.int32)
        for j in range(tile_cols):
            col_chain = jnp.where(sub == j, asym[first_col + j], col_chain)
        reach = bins // 2 - 1
        turned_weight = bias_weight[...]
        for t in range(stripes):
            hots, rows = [], []
            for q in range(fold):
                i = q * stripes + t
                offset = jnp.clip(first_row + i - first_col - sub, -reach, reach) + reach
                bin_ids = jnp.where(col_chain == asym[first_row + i], offset, bins - 1)
                hots.append(jnp.where(bin_ids == lane, 1.0, 0.0).astype(jnp.bfloat16))
                rows.append(pair[i].astype(jnp.float32))
            summed = jnp.concatenate(rows, axis=0) + jnp.dot(
                jnp.concatenate(hots, axis=0), rel[...], preferred_element_type=jnp.float32
            )
            normed_pair = normalize(summed, pair_gain[...]).astype(jnp.bfloat16)
            projected = lax.dot_general(
                turned_weight, normed_pair, (((1,), (1,)), ((), ())), preferred_element_type=jnp.float32
            )
            bias_send[pl.ds(t, all_heads, stride=stripes), :] = projected

    with mark("loads"):
        for name in ("tok", "ow", "qkv", "token_gain", "valid"):
            loads[name].wait()
    with mark("barrier"):
        pl.semaphore_wait(barrier, greeted)

    def ow_piece(source):
        first = aligned((here[0] * p_samp + here[2]) * piece_rows, piece_rows)
        start = aligned(here[1] * piece_cols, piece_cols)
        return ow.at[source, pl.ds(first, piece_rows), pl.ds(start, piece_cols)]

    def send_ow():
        for k in range(1, n_row):
            send(ow_piece(me), ow_piece(me), sent.at[2], ow_got.at[0, k - 1], {"row": row_peer(k)})

    shifts = [
        (a, b, c) for a in range(p_job) for b in range(p_col) for c in range(p_samp) if a or b or c
    ]

    def spread_ow(k):
        piece = ow_piece(row_source(k))
        arrive(piece, ow_got.at[0, k - 1])
        for shift in shifts:
            device = {
                name: lax.rem(spot + step, size)
                for name, spot, step, size in zip(("job", "col", "samp"), here, shift, cuts)
                if step
            }
            send(piece, piece, sent.at[2], ow_got.at[1, k - 1], device)

    def take_ow(k):
        if pieces > 1:
            arrive(ow.at[row_source(k), pl.ds(0, out_rows - out_rows // pieces)], ow_got.at[1, k - 1])

    has_right, has_left = me < n_row - 1, me > 0
    edge = jnp.logical_or(me == 0, me == n_row - 1)
    def push_tokens(s, source, rightward):
        send(
            tok.at[s, source],
            tok.at[s, source],
            tok_sent.at[0 if rightward else 1, source],
            tok_got.at[s, source],
            {"row": jnp.minimum(me + 1, n_row - 1) if rightward else jnp.maximum(me - 1, 0)},
        )

    def send_tokens(s):
        @pl.when(has_right)
        def _():
            push_tokens(s, me, True)

        @pl.when(has_left)
        def _():
            push_tokens(s, me, False)

    def take_tokens(s, distance):
        @pl.when(me >= distance)
        def _():
            source = jnp.maximum(me - distance, 0)
            arrive(tok.at[s, source], tok_got.at[s, source])

            @pl.when(has_right)
            def _():
                push_tokens(s, source, True)

        @pl.when(me + distance < n_row)
        def _():
            source = jnp.minimum(me + distance, n_row - 1)
            arrive(tok.at[s, source], tok_got.at[s, source])

            @pl.when(has_left)
            def _():
                push_tokens(s, source, False)

    def bias_part(target):
        return bias_send.at[
            pl.ds(pl.multiple_of(target * part_rows, part_rows), part_rows)
        ]

    def spread_bias(k):
        place = bias_recv.at[row_source(k) * n_plane + plane]
        held = place if k else bias_part(me)
        for m in range(1, n_plane):
            other = lax.rem(plane + m, n_plane)
            send(
                held,
                place,
                sent.at[1],
                bias_got.at[n_row - 1],
                {"col": lax.div(other, n_samp), "samp": lax.rem(other, n_samp)},
            )

    def send_bias():
        for k in range(1, n_row):
            target = row_peer(k)
            send(
                bias_part(target),
                bias_recv.at[me * n_plane + plane],
                sent.at[1],
                bias_got.at[k - 1],
                {"row": target},
            )
        spread_bias(0)

    def pass_bias(k):
        arrive(bias_recv.at[row_source(k) * n_plane + plane], bias_got.at[k - 1])
        spread_bias(k)

    def take_bias():
        if n_plane > 1:
            arrive(bias_recv.at[pl.ds(0, n_row * (n_plane - 1))], bias_got.at[n_row - 1])

    own_bias = pltpu.make_async_copy(
        bias_part(me), bias_recv.at[me * n_plane + plane], local_sem.at[11]
    )

    head_of_lane = lax.broadcasted_iota(jnp.int32, (total, local_width), 1)
    head_masks = [
        jnp.logical_and(head_of_lane >= h * HEAD_DIM, head_of_lane < (h + 1) * HEAD_DIM)
        for h in range(local_heads)
    ]
    scale = 1.0 / math.sqrt(HEAD_DIM)

    def project(sources, chosen=slice(None)):
        rows = tok[chosen, sources].reshape(-1, width).astype(jnp.float32)
        normed = normalize(rows, token_gain[...]).astype(jnp.bfloat16)
        for index, target in enumerate((query, key, value)):
            done = lax.dot_general(
                normed, qkv[index], (((1,), (1,)), ((), ())), preferred_element_type=jnp.float32
            ).astype(jnp.bfloat16)
            target[chosen, sources] = done.reshape(target[chosen, sources].shape)

    def attend(s):
        whole = (total, local_width)
        keys = key[s].reshape(whole).astype(jnp.float32)
        values = value[s].reshape(whole).astype(jnp.float32)
        keys = jnp.concatenate(
            [jnp.where(mask, keys, 0.0).astype(jnp.bfloat16) for mask in head_masks], axis=0
        )
        values = jnp.concatenate(
            [jnp.where(mask, values, 0.0).astype(jnp.bfloat16) for mask in head_masks], axis=0
        )
        scores = lax.dot_general(
            query[s].reshape(whole), keys, (((1,), (1,)), ((), ())), preferred_element_type=jnp.float32
        )
        probs = []
        for h in range(local_heads):
            span = slice(h * total, (h + 1) * total)
            logits = scores[:, span] * scale + bias[:, span]
            weights = jnp.exp(logits - jnp.max(logits, axis=-1, keepdims=True))
            inverse = 1.0 / jnp.sum(weights, axis=-1, keepdims=True)
            probs.append((weights * inverse).astype(jnp.bfloat16))
        mixed = jnp.dot(
            jnp.concatenate(probs, axis=1), values, preferred_element_type=jnp.float32
        ).astype(jnp.bfloat16)
        attended[s] = mixed.reshape(n_row, token_rows, local_width)

    def give(s):
        for d in range(1, n_row):
            target = row_peer(d)
            send(attended.at[s, target], heads_in.at[me * samples + s], sent.at[0], att_got.at[0], {"row": target})
        heads_in[me * samples + s] = attended[s, me]

    def take_attended():
        arrive(heads_in.at[pl.ds(0, (n_row - 1) * samples)], att_got.at[0])

    def build_bias():
        lanes_at = lax.broadcasted_iota(jnp.int32, (part_rows, LANES), 1)
        for tile in range(total // LANES):
            padded = lanes_at[:stripes] + tile * LANES >= valid[0]
            for r in range(n_row):
                parts = [bias_recv[r * n_plane + tile * fold + m] for m in range(fold)]
                for q in range(fold):
                    whole = None
                    for m in range(fold):
                        shift = ((m - q) % fold) * tile_cols
                        turned = pltpu.roll(parts[m], shift, 1) if shift else parts[m]
                        whole = (
                            turned
                            if whole is None
                            else jnp.where(lanes_at >= m * tile_cols, turned, whole)
                        )
                    at = r * tile_rows + q * stripes
                    for h in range(local_heads):
                        bias[
                            at : at + stripes,
                            h * total + tile * LANES : h * total + (tile + 1) * LANES,
                        ] = jnp.where(padded, -1e30, whole[h * stripes : (h + 1) * stripes])

    everything = slice(None)
    send_bias()
    send_ow()
    own_bias.start()
    for s in range(samples):
        send_tokens(s)

    @pl.when(edge)
    def _():
        with mark("project"):
            project(me)

    with mark("bias0"):
        for k in range(1, n_row):
            pass_bias(k)
    with mark("ow0"):
        for k in range(1, n_row):
            spread_ow(k)
    for distance in range(1, n_row - 1):
        with mark("tokens"):
            for s in range(samples):
                take_tokens(s, distance)

        @pl.when(edge)
        def _():
            with mark("project"):
                project(jnp.where(me == 0, distance, me - distance))

    def prepare_bias():
        with mark("bias2"):
            own_bias.wait()
            take_bias()
        with mark("build"):
            build_bias()

    def finish_sample(s):
        with mark("attend"):
            attend(s)
        with mark("give"):
            give(s)

    @pl.when(edge)
    def _():
        prepare_bias()
        for s in range(samples):
            with mark("tokense"):
                take_tokens(s, n_row - 1)
            with mark("project"):
                project(n_row - 1 - me, slice(s, s + 1))
            finish_sample(s)

    @pl.when(jnp.logical_not(edge))
    def _():
        for s in range(samples):
            with mark("tokensi"):
                take_tokens(s, n_row - 1)
        with mark("projecti"):
            project(slice(None))
        prepare_bias()
        for s in range(samples):
            finish_sample(s)

    with mark("ow3"):
        for k in range(1, n_row):
            take_ow(k)
    with mark("attwait"):
        take_attended()

    with mark("product"):
        result = tok[:, me].reshape(samples * token_rows, width).astype(jnp.float32)
        product = None
        for r in range(n_row):
            flat = heads_in[r * samples : (r + 1) * samples].reshape(samples * token_rows, local_width)
            term = jnp.dot(flat, ow[r], preferred_element_type=jnp.float32)
            product = term if product is None else product + term
        out[...] = (result + product).astype(out.dtype).reshape(samples, token_rows, width)

    with mark("fin"):
        for source in range(n_row):
            for rightward in (True, False):

                @pl.when(jnp.logical_and(source <= me, has_right) if rightward else jnp.logical_and(source >= me, has_left))
                def _():
                    awaiting(tok.at[:, source], tok_sent.at[0 if rightward else 1, source]).wait_send()

        awaiting(bias_recv.at[pl.ds(0, n_row * n_plane - 1)], sent.at[1]).wait_send()
        awaiting(attended.at[:, pl.ds(0, n_row - 1)], sent.at[0]).wait_send()
        awaiting(ow.at[pl.ds(0, n_row - 1)], sent.at[2]).wait_send()


def per_device(
    axes,
    pair_repr,
    asym_id,
    valid_len,
    rel_embed,
    pair_gain,
    bias_weight,
    tokens,
    token_gain,
    qkv_weight,
    out_weight,
):
    n_job, n_row, n_col, n_samp = axes
    samples, token_rows, width = tokens.shape
    total = n_row * token_rows
    n_plane = n_col * n_samp
    heads = bias_weight.shape[1]
    local_heads = heads // n_row
    tile_rows, tile_cols, channels = pair_repr.shape
    local_width = qkv_weight.shape[-1]
    out_rows = out_weight.shape[1]
    cut_rows = out_rows % (16 * n_job * n_samp) == 0
    cut_cols = width % (LANES * n_col) == 0
    cuts = (n_job if cut_rows else 1, n_col if cut_cols else 1, n_samp if cut_rows else 1)
    stripes = tile_rows // (LANES // tile_cols)
    part_rows = local_heads * stripes
    bf16, f32 = jnp.bfloat16, jnp.float32
    dma = pltpu.SemaphoreType.DMA
    any_spec = pl.BlockSpec(memory_space=pltpu.HBM)
    return pl.pallas_call(
        functools.partial(kernel, axes, cuts),
        out_shape=jax.ShapeDtypeStruct(tokens.shape, tokens.dtype),
        in_specs=[any_spec] * 10,
        out_specs=pl.BlockSpec(memory_space=pltpu.VMEM),
        scratch_shapes=[
            pltpu.SMEM(asym_id.shape, jnp.int32),
            pltpu.SMEM(valid_len.shape, jnp.int32),
            pltpu.VMEM(pair_repr.shape, bf16),
            pltpu.VMEM(rel_embed.shape, bf16),
            pltpu.VMEM((1, channels), f32),
            pltpu.VMEM(bias_weight.shape[::-1], bf16),
            pltpu.VMEM(token_gain.shape, f32),
            pltpu.VMEM((3, local_width, width), bf16),
            pltpu.VMEM((samples, n_row, token_rows, width), bf16),
            pltpu.VMEM((n_row, out_rows, width), bf16),
            pltpu.VMEM((heads * stripes, LANES), f32),
            pltpu.VMEM((n_row * n_plane, part_rows, LANES), f32),
            pltpu.VMEM((total, local_heads * total), f32),
            pltpu.VMEM((samples, n_row, token_rows, local_width), bf16),
            pltpu.VMEM((samples, n_row, token_rows, local_width), bf16),
            pltpu.VMEM((samples, n_row, token_rows, local_width), bf16),
            pltpu.VMEM((samples, n_row, token_rows, local_width), bf16),
            pltpu.VMEM((n_row * samples, token_rows, local_width), bf16),
            dma((12,)),
            dma((samples, n_row)),
            dma((2, n_row)),
            dma((n_row,)),
            dma((2, n_row - 1)),
            dma((1,)),
            dma((3,)),
        ],
        compiler_params=pltpu.CompilerParams(
            collective_id=0, has_side_effects=True, vmem_limit_bytes=24 * 1024 * 1024
        ),
    )(
        *(
            operand if operand is valid_len else pltpu.with_memory_space_constraint(operand, pltpu.HBM)
            for operand in (
                asym_id,
                valid_len,
                pair_repr,
                rel_embed,
                pair_gain.reshape(1, channels),
                bias_weight.T,
                tokens,
                token_gain,
                jnp.swapaxes(qkv_weight, 2, 3),
                out_weight,
            )
        )
    )


def solution(mesh):
    axes = tuple(mesh.shape[name] for name in ("job", "row", "col", "samp"))
    return jax.shard_map(
        functools.partial(per_device, axes),
        mesh=mesh,
        in_specs=(
            P(("job", "row"), ("col", "samp"), None),
            P("job"),
            P("job"),
            P(),
            P(),
            P(),
            P(("job", "col", "samp"), "row", None),
            P(),
            P(None, None, None, "row"),
            P(None, "row", None),
        ),
        out_specs=P(("job", "col", "samp"), "row", None),
        check_vma=False,
    )
```

```python
import contextlib
import functools
import math

import jax
import jax.numpy as jnp
from jax import lax
from jax.experimental import pallas as pl
from jax.experimental.pallas import tpu as pltpu
from jax.sharding import PartitionSpec as P

HEAD_DIM = 48
EPSILON = 1e-05
LANES = 128
MESH = pl.DeviceIdType.MESH
mark = contextlib.nullcontext


def normalize(values, gain_vector):
    average = jnp.mean(values, axis=-1, keepdims=True)
    centered = values - average
    variance = jnp.mean(centered * centered, axis=-1, keepdims=True)
    return centered * lax.rsqrt(variance + EPSILON) * gain_vector


def back(position, shift, size):
    return lax.rem(position + (size - shift), size) if shift else position


def aligned(value, unit):
    return value if isinstance(value, int) else pl.multiple_of(value, unit)


def kernel(
    axes,
    cuts,
    asym_hbm,
    valid_hbm,
    pair_hbm,
    rel_hbm,
    pair_gain_hbm,
    bias_weight_hbm,
    tokens_hbm,
    token_gain_hbm,
    qkv_hbm,
    out_weight_hbm,
    out,
    asym,
    valid,
    pair,
    rel,
    pair_gain,
    bias_weight,
    token_gain,
    qkv,
    tok,
    ow,
    bias_send,
    bias_recv,
    bias,
    query,
    key,
    value,
    attended,
    heads_in,
    local_sem,
    tok_got,
    tok_sent,
    bias_got,
    ow_got,
    ow_sent,
    att_got,
    sent,
    greeting,
):
    n_job, n_row, n_col, n_samp = axes
    job, me = lax.axis_index("job"), lax.axis_index("row")
    col, samp = lax.axis_index("col"), lax.axis_index("samp")
    samples, token_rows, width = tokens_hbm.shape
    total = n_row * token_rows
    tile_rows, tile_cols, channels = pair.shape
    bins = rel.shape[0]
    plane = col * n_samp + samp
    all_heads = bias_weight.shape[0]
    local_heads = all_heads // n_row
    local_width = local_heads * HEAD_DIM
    fold = LANES // tile_cols
    stripes = tile_rows // fold
    part_rows = bias_recv.shape[1]
    out_rows = ow.shape[1]
    n_plane = n_col * n_samp
    p_job, p_col = cuts
    pieces = p_job * p_col
    piece_rows, piece_cols = out_rows // p_job, width // p_col
    relay = samp == n_samp - 1

    def row_peer(k):
        return lax.rem(me + k, n_row)

    def row_source(k):
        return back(me, k, n_row)

    def send(source, target, left, got, device):
        pltpu.make_async_remote_copy(
            src_ref=source,
            dst_ref=target,
            send_sem=left,
            recv_sem=got,
            device_id=device,
            device_id_type=MESH,
        ).start()

    def awaiting(ref, semaphore):
        return pltpu.make_async_remote_copy(
            src_ref=ref,
            dst_ref=ref,
            send_sem=semaphore,
            recv_sem=semaphore,
            device_id={"row": row_peer(1)},
            device_id_type=MESH,
        )

    def arrive(ref, semaphore):
        awaiting(ref, semaphore).wait_recv()

    has_right, has_left = me < n_row - 1, me > 0
    edge = jnp.logical_or(me == 0, me == n_row - 1)

    def greet(semaphore):
        for name, spot, size in (("col", col, n_col), ("samp", samp, n_samp), ("job", job, p_job)):
            for k in range(1, size):
                device = {name: lax.rem(spot + k, size)}
                pl.semaphore_signal(semaphore, inc=1, device_id=device, device_id_type=MESH)

        @pl.when(has_right)
        def _():
            device = {"row": jnp.minimum(me + 1, n_row - 1)}
            pl.semaphore_signal(semaphore, inc=1, device_id=device, device_id_type=MESH)

        @pl.when(has_left)
        def _():
            device = {"row": jnp.maximum(me - 1, 0)}
            pl.semaphore_signal(semaphore, inc=1, device_id=device, device_id_type=MESH)

    def await_greetings(semaphore):
        others = (n_col - 1) + (n_samp - 1) + (p_job - 1)
        pl.semaphore_wait(semaphore, others + jnp.where(edge, 1, 2))

    rounds = greeting.shape[0]
    barrier = pltpu.get_barrier_semaphore()
    greet(barrier)

    loads = {}
    for index, (name, source, target) in enumerate(
        (
            ("asym", asym_hbm, asym),
            ("pair", pair_hbm, pair),
            ("rel", rel_hbm, rel),
            ("pair_gain", pair_gain_hbm, pair_gain),
            ("bias_weight", bias_weight_hbm, bias_weight),
            ("qkv", qkv_hbm.at[0], qkv),
            ("token_gain", token_gain_hbm, token_gain),
            ("ow", out_weight_hbm.at[0], ow.at[me]),
            ("valid", valid_hbm, valid),
        )
    ):
        loads[name] = pltpu.make_async_copy(source, target, local_sem.at[index])
    loads["tok"] = pltpu.make_async_copy(tokens_hbm, tok.at[:, me], local_sem.at[9])
    for name in ("tok", "asym", "pair", "rel", "pair_gain", "bias_weight", "qkv", "token_gain", "ow", "valid"):
        loads[name].start()

    def ow_piece(source, a, b):
        first = aligned(lax.rem(job + a, n_job) * piece_rows if p_job > 1 else 0, piece_rows)
        start = aligned(lax.rem(col + b, n_col) * piece_cols if p_col > 1 else 0, piece_cols)
        return ow.at[source, pl.ds(first, piece_rows), pl.ds(start, piece_cols)]

    chips = [(a, b) for a in range(p_job) for b in range(p_col)]

    def send_ow():
        for k in range(1, n_row):
            send(ow_piece(me, 0, 0), ow_piece(me, 0, 0), sent.at[2], ow_got.at[0, k - 1], {"row": row_peer(k)})

    def pair_ow(k, a, b):
        piece = ow_piece(row_source(k), a, b)
        for e in range(1, n_samp):
            device = {"samp": lax.rem(samp + e, n_samp)}
            send(piece, piece, ow_sent.at[e - 1], ow_got.at[2, k - 1], device)

    def spread_ow(k):
        piece = ow_piece(row_source(k), 0, 0)
        arrive(piece, ow_got.at[0, k - 1])
        for a, b in chips[1:]:
            device = {
                name: lax.rem(spot + step, size)
                for name, spot, step, size in (("job", job, a, n_job), ("col", col, b, n_col))
                if step
            }
            send(piece, piece, sent.at[2], ow_got.at[1, k - 1], device)
        pair_ow(k, 0, 0)

    def collect_ow(k):
        if pieces > 1:
            arrive(ow.at[row_source(k), pl.ds(0, out_rows - out_rows // pieces)], ow_got.at[1, k - 1])
            for a, b in chips[1:]:
                pair_ow(k, a, b)

    def take_ow(k):
        arrive(ow.at[row_source(k)], ow_got.at[2, k - 1])

    def push_tokens(s, source, rightward):
        send(
            tok.at[s, source],
            tok.at[s, source],
            tok_sent.at[0 if rightward else 1, source],
            tok_got.at[s, source],
            {"row": jnp.minimum(me + 1, n_row - 1) if rightward else jnp.maximum(me - 1, 0)},
        )

    def send_tokens(s):
        @pl.when(has_right)
        def _():
            push_tokens(s, me, True)

        @pl.when(has_left)
        def _():
            push_tokens(s, me, False)

    def take_tokens(s, distance):
        @pl.when(me >= distance)
        def _():
            source = jnp.maximum(me - distance, 0)
            arrive(tok.at[s, source], tok_got.at[s, source])

            @pl.when(has_right)
            def _():
                push_tokens(s, source, True)

        @pl.when(me + distance < n_row)
        def _():
            source = jnp.minimum(me + distance, n_row - 1)
            arrive(tok.at[s, source], tok_got.at[s, source])

            @pl.when(has_left)
            def _():
                push_tokens(s, source, False)

    def bias_part(target):
        return bias_send.at[
            pl.ds(pl.multiple_of(target * part_rows, part_rows), part_rows)
        ]

    def spread_bias(k):
        place = bias_recv.at[row_source(k) * n_plane + plane]
        held = place if k else bias_part(me)
        for m in range(1, n_plane):
            other = lax.rem(plane + m, n_plane)
            send(
                held,
                place,
                sent.at[1],
                bias_got.at[n_row - 1],
                {"col": lax.div(other, n_samp), "samp": lax.rem(other, n_samp)},
            )

    def send_bias():
        for k in range(1, n_row):
            target = row_peer(k)
            send(
                bias_part(target),
                bias_recv.at[me * n_plane + plane],
                sent.at[1],
                bias_got.at[k - 1],
                {"row": target},
            )
        spread_bias(0)

    def pass_bias(k):
        arrive(bias_recv.at[row_source(k) * n_plane + plane], bias_got.at[k - 1])
        spread_bias(k)

    def take_bias():
        if n_plane > 1:
            arrive(bias_recv.at[pl.ds(0, n_row * (n_plane - 1))], bias_got.at[n_row - 1])

    own_bias = pltpu.make_async_copy(
        bias_part(me), bias_recv.at[me * n_plane + plane], local_sem.at[11]
    )

    head_of_lane = lax.broadcasted_iota(jnp.int32, (total, local_width), 1)
    head_masks = [
        jnp.logical_and(head_of_lane >= h * HEAD_DIM, head_of_lane < (h + 1) * HEAD_DIM)
        for h in range(local_heads)
    ]
    scale = 1.0 / math.sqrt(HEAD_DIM)

    def project(sources, chosen=slice(None)):
        rows = tok[chosen, sources].reshape(-1, width).astype(jnp.float32)
        normed = normalize(rows, token_gain[...]).astype(jnp.bfloat16)
        for index, target in enumerate((query, key, value)):
            done = lax.dot_general(
                normed, qkv[index], (((1,), (1,)), ((), ())), preferred_element_type=jnp.float32
            ).astype(jnp.bfloat16)
            target[chosen, sources] = done.reshape(target[chosen, sources].shape)

    def attend(s):
        whole = (total, local_width)
        keys = key[s].reshape(whole).astype(jnp.float32)
        values = value[s].reshape(whole).astype(jnp.float32)
        keys = jnp.concatenate(
            [jnp.where(mask, keys, 0.0).astype(jnp.bfloat16) for mask in head_masks], axis=0
        )
        values = jnp.concatenate(
            [jnp.where(mask, values, 0.0).astype(jnp.bfloat16) for mask in head_masks], axis=0
        )
        scores = lax.dot_general(
            query[s].reshape(whole), keys, (((1,), (1,)), ((), ())), preferred_element_type=jnp.float32
        )
        probs = []
        for h in range(local_heads):
            span = slice(h * total, (h + 1) * total)
            logits = scores[:, span] * scale + bias[:, span]
            weights = jnp.exp(logits - jnp.max(logits, axis=-1, keepdims=True))
            inverse = 1.0 / jnp.sum(weights, axis=-1, keepdims=True)
            probs.append((weights * inverse).astype(jnp.bfloat16))
        mixed = jnp.dot(
            jnp.concatenate(probs, axis=1), values, preferred_element_type=jnp.float32
        ).astype(jnp.bfloat16)
        attended[s] = mixed.reshape(n_row, token_rows, local_width)

    def give(s):
        for d in range(1, n_row):
            target = row_peer(d)
            send(attended.at[s, target], heads_in.at[me * samples + s], sent.at[0], att_got.at[0], {"row": target})
        heads_in[me * samples + s] = attended[s, me]

    def take_attended():
        arrive(heads_in.at[pl.ds(0, (n_row - 1) * samples)], att_got.at[0])

    def build_bias():
        lanes_at = lax.broadcasted_iota(jnp.int32, (part_rows, LANES), 1)
        for tile in range(total // LANES):
            padded = lanes_at[:stripes] + tile * LANES >= valid[0]
            for r in range(n_row):
                parts = [bias_recv[r * n_plane + tile * fold + m] for m in range(fold)]
                for q in range(fold):
                    whole = None
                    for m in range(fold):
                        shift = ((m - q) % fold) * tile_cols
                        turned = pltpu.roll(parts[m], shift, 1) if shift else parts[m]
                        whole = (
                            turned
                            if whole is None
                            else jnp.where(lanes_at >= m * tile_cols, turned, whole)
                        )
                    at = r * tile_rows + q * stripes
                    for h in range(local_heads):
                        bias[
                            at : at + stripes,
                            h * total + tile * LANES : h * total + (tile + 1) * LANES,
                        ] = jnp.where(padded, -1e30, whole[h * stripes : (h + 1) * stripes])

    everything = slice(None)
    with mark("tokload"):
        loads["tok"].wait()
    with mark("barrier"):
        await_greetings(barrier)

    early = 2
    for s in range(early):
        send_tokens(s)

    @pl.when(jnp.logical_not(relay))
    def _():
        for s in range(early, samples):
            send_tokens(s)

    with mark("pairload"):
        for name in ("asym", "pair", "rel", "pair_gain", "bias_weight"):
            loads[name].wait()
    first_row, first_col = me * tile_rows, plane * tile_cols
    sub = lax.broadcasted_iota(jnp.int32, (tile_cols, LANES), 0)
    lane = lax.broadcasted_iota(jnp.int32, (tile_cols, LANES), 1)
    with mark("pairprep"):
        col_chain = jnp.zeros((tile_cols, LANES), jnp.int32)
        for j in range(tile_cols):
            col_chain = jnp.where(sub == j, asym[first_col + j], col_chain)
        reach = bins // 2 - 1
        turned_weight = bias_weight[...]
    def pair_stripes(first, last):
        for t in range(first, last):
            hots, rows = [], []
            for q in range(fold):
                i = q * stripes + t
                offset = jnp.clip(first_row + i - first_col - sub, -reach, reach) + reach
                bin_ids = jnp.where(col_chain == asym[first_row + i], offset, bins - 1)
                hots.append(jnp.where(bin_ids == lane, 1.0, 0.0).astype(jnp.bfloat16))
                rows.append(pair[i].astype(jnp.float32))
            summed = jnp.concatenate(rows, axis=0) + jnp.dot(
                jnp.concatenate(hots, axis=0), rel[...], preferred_element_type=jnp.float32
            )
            normed_pair = normalize(summed, pair_gain[...]).astype(jnp.bfloat16)
            projected = lax.dot_general(
                turned_weight, normed_pair, (((1,), (1,)), ((), ())), preferred_element_type=jnp.float32
            )
            bias_send[pl.ds(t, all_heads, stride=stripes), :] = projected

    for r in range(rounds):
        greet(greeting.at[r])
        with mark("pair"):
            pair_stripes(r * stripes // rounds, (r + 1) * stripes // rounds)
        with mark("greeting"):
            await_greetings(greeting.at[r])

    with mark("loads"):
        for name in ("ow", "qkv", "token_gain", "valid"):
            loads[name].wait()
    send_bias()
    own_bias.start()

    @pl.when(relay)
    def _():
        send_ow()
        for s in range(early, samples):
            send_tokens(s)

    @pl.when(edge)
    def _():
        with mark("project"):
            project(me)

    def step(distance):
        for s in range(samples):
            with mark("tokens"):
                take_tokens(s, distance)
            if distance == 1 and s == 1:

                @pl.when(relay)
                def _():
                    with mark("ow0"):
                        for k in range(1, n_row):
                            spread_ow(k)

        @pl.when(edge)
        def _():
            with mark("project"):
                project(jnp.where(me == 0, distance, me - distance))

    def first_bias():
        with mark("bias0"):
            for k in range(1, n_row):
                pass_bias(k)

    @pl.when(relay)
    def _():
        first_bias()

    if n_row > 2:
        step(1)

    @pl.when(jnp.logical_not(relay))
    def _():
        first_bias()

    for distance in range(2, n_row - 1):
        step(distance)

    def relay_ow():
        @pl.when(relay)
        def _():
            with mark("ow1"):
                for k in range(1, n_row):
                    collect_ow(k)

    def prepare_bias():
        with mark("bias2"):
            own_bias.wait()
            take_bias()
        with mark("build"):
            build_bias()

    def finish_samples(first, last):
        with mark("attend"):
            for s in range(first, last):
                attend(s)
        with mark("give"):
            for s in range(first, last):
                give(s)

    batch = max(samples // 2, 1)
    batches = [(first, min(first + batch, samples)) for first in range(0, samples, batch)]

    @pl.when(edge)
    def _():
        prepare_bias()
        for first, last in batches:
            with mark("tokense"):
                for s in range(first, last):
                    take_tokens(s, n_row - 1)
            with mark("project"):
                project(n_row - 1 - me, slice(first, last))
            finish_samples(first, last)
            if first == 0:
                relay_ow()

    @pl.when(jnp.logical_not(edge))
    def _():
        for s in range(samples):
            with mark("tokensi"):
                take_tokens(s, n_row - 1)
        with mark("projecti"):
            project(slice(None))
        prepare_bias()
        for first, last in batches:
            finish_samples(first, last)
        relay_ow()

    @pl.when(jnp.logical_not(relay))
    def _():
        with mark("ow3"):
            for k in range(1, n_row):
                take_ow(k)

    with mark("attwait"):
        take_attended()

    with mark("product"):
        result = tok[:, me].reshape(samples * token_rows, width).astype(jnp.float32)
        product = None
        for r in range(n_row):
            flat = heads_in[r * samples : (r + 1) * samples].reshape(samples * token_rows, local_width)
            term = jnp.dot(flat, ow[r], preferred_element_type=jnp.float32)
            product = term if product is None else product + term
        out[...] = (result + product).astype(out.dtype).reshape(samples, token_rows, width)

    with mark("fin"):
        for source in range(n_row):
            for rightward in (True, False):

                @pl.when(jnp.logical_and(source <= me, has_right) if rightward else jnp.logical_and(source >= me, has_left))
                def _():
                    awaiting(tok.at[:, source], tok_sent.at[0 if rightward else 1, source]).wait_send()

        awaiting(bias_recv.at[pl.ds(0, n_row * n_plane - 1)], sent.at[1]).wait_send()
        awaiting(attended.at[:, pl.ds(0, n_row - 1)], sent.at[0]).wait_send()

        @pl.when(relay)
        def _():
            awaiting(ow.at[pl.ds(0, n_row - 1)], sent.at[2]).wait_send()
            for e in range(1, n_samp):
                awaiting(ow.at[pl.ds(0, n_row - 1)], ow_sent.at[e - 1]).wait_send()


def per_device(
    axes,
    pair_repr,
    asym_id,
    valid_len,
    rel_embed,
    pair_gain,
    bias_weight,
    tokens,
    token_gain,
    qkv_weight,
    out_weight,
):
    n_job, n_row, n_col, n_samp = axes
    samples, token_rows, width = tokens.shape
    total = n_row * token_rows
    n_plane = n_col * n_samp
    heads = bias_weight.shape[1]
    local_heads = heads // n_row
    tile_rows, tile_cols, channels = pair_repr.shape
    local_width = qkv_weight.shape[-1]
    out_rows = out_weight.shape[1]
    cuts = (1 if out_rows % (16 * n_job) else n_job, 1 if width % (LANES * n_col) else n_col)
    stripes = tile_rows // (LANES // tile_cols)
    part_rows = local_heads * stripes
    bf16, f32 = jnp.bfloat16, jnp.float32
    dma = pltpu.SemaphoreType.DMA
    any_spec = pl.BlockSpec(memory_space=pltpu.HBM)
    return pl.pallas_call(
        functools.partial(kernel, axes, cuts),
        out_shape=jax.ShapeDtypeStruct(tokens.shape, tokens.dtype),
        in_specs=[any_spec] * 10,
        out_specs=pl.BlockSpec(memory_space=pltpu.VMEM),
        scratch_shapes=[
            pltpu.SMEM(asym_id.shape, jnp.int32),
            pltpu.SMEM(valid_len.shape, jnp.int32),
            pltpu.VMEM(pair_repr.shape, bf16),
            pltpu.VMEM(rel_embed.shape, bf16),
            pltpu.VMEM((1, channels), f32),
            pltpu.VMEM(bias_weight.shape[::-1], bf16),
            pltpu.VMEM(token_gain.shape, f32),
            pltpu.VMEM((3, local_width, width), bf16),
            pltpu.VMEM((samples, n_row, token_rows, width), bf16),
            pltpu.VMEM((n_row, out_rows, width), bf16),
            pltpu.VMEM((heads * stripes, LANES), f32),
            pltpu.VMEM((n_row * n_plane, part_rows, LANES), f32),
            pltpu.VMEM((total, local_heads * total), f32),
            pltpu.VMEM((samples, n_row, token_rows, local_width), bf16),
            pltpu.VMEM((samples, n_row, token_rows, local_width), bf16),
            pltpu.VMEM((samples, n_row, token_rows, local_width), bf16),
            pltpu.VMEM((samples, n_row, token_rows, local_width), bf16),
            pltpu.VMEM((n_row * samples, token_rows, local_width), bf16),
            dma((12,)),
            dma((samples, n_row)),
            dma((2, n_row)),
            dma((n_row,)),
            dma((3, n_row - 1)),
            dma((max(n_samp - 1, 1),)),
            dma((1,)),
            dma((3,)),
            pltpu.SemaphoreType.REGULAR((max(n_row - 2, 2),)),
        ],
        compiler_params=pltpu.CompilerParams(
            collective_id=0, has_side_effects=True, vmem_limit_bytes=24 * 1024 * 1024
        ),
    )(
        *(
            operand if operand is valid_len else pltpu.with_memory_space_constraint(operand, pltpu.HBM)
            for operand in (
                asym_id,
                valid_len,
                pair_repr,
                rel_embed,
                pair_gain.reshape(1, channels),
                bias_weight.T,
                tokens,
                token_gain,
                jnp.swapaxes(qkv_weight, 2, 3),
                out_weight,
            )
        )
    )


def solution(mesh):
    axes = tuple(mesh.shape[name] for name in ("job", "row", "col", "samp"))
    return jax.shard_map(
        functools.partial(per_device, axes),
        mesh=mesh,
        in_specs=(
            P(("job", "row"), ("col", "samp"), None),
            P("job"),
            P("job"),
            P(),
            P(),
            P(),
            P(("job", "col", "samp"), "row", None),
            P(),
            P(None, None, None, "row"),
            P(None, "row", None),
        ),
        out_specs=P(("job", "col", "samp"), "row", None),
        check_vma=False,
    )
```

```python
import contextlib
import functools
import math

import jax
import jax.numpy as jnp
from jax import lax
from jax.experimental import pallas as pl
from jax.experimental.pallas import tpu as pltpu
from jax.sharding import PartitionSpec as P

HEAD_DIM = 48
EPSILON = 1e-05
LANES = 128
MESH = pl.DeviceIdType.MESH
mark = contextlib.nullcontext


def normalize(values, gain_vector):
    average = jnp.mean(values, axis=-1, keepdims=True)
    centered = values - average
    variance = jnp.mean(centered * centered, axis=-1, keepdims=True)
    return centered * lax.rsqrt(variance + EPSILON) * gain_vector


def back(position, shift, size):
    return lax.rem(position + (size - shift), size) if shift else position


def aligned(value, unit):
    return value if isinstance(value, int) else pl.multiple_of(value, unit)


def kernel(
    axes,
    cuts,
    asym_hbm,
    valid_hbm,
    pair_hbm,
    rel_hbm,
    pair_gain_hbm,
    bias_weight_hbm,
    tokens_hbm,
    token_gain_hbm,
    qkv_hbm,
    out_weight_hbm,
    out,
    asym,
    valid,
    pair,
    rel,
    pair_gain,
    bias_weight,
    token_gain,
    qkv,
    own,
    tok,
    ow,
    bias_send,
    bias_recv,
    bias,
    query,
    key,
    value,
    attended,
    heads_in,
    total_sum,
    local_sem,
    tok_got,
    tok_sent,
    bias_got,
    ow_got,
    ow_sent,
    att_got,
    sent,
    greeting,
):
    n_job, n_row, n_col, n_samp = axes
    job, me = lax.axis_index("job"), lax.axis_index("row")
    col, samp = lax.axis_index("col"), lax.axis_index("samp")
    samples, token_rows, width = tokens_hbm.shape
    total = n_row * token_rows
    tile_rows, tile_cols, channels = pair.shape
    bins = rel.shape[0]
    plane = col * n_samp + samp
    all_heads = bias_weight.shape[0]
    local_heads = all_heads // n_row
    local_width = local_heads * HEAD_DIM
    fold = LANES // tile_cols
    stripes = tile_rows // fold
    part_rows = bias_recv.shape[1]
    out_rows = ow.shape[1]
    n_plane = n_col * n_samp
    p_job, p_col = cuts
    pieces = p_job * p_col
    piece_rows, piece_cols = out_rows // p_job, width // p_col
    relay = samp == n_samp - 1

    def row_peer(k):
        return lax.rem(me + k, n_row)

    def row_source(k):
        return back(me, k, n_row)

    def send(source, target, left, got, device):
        pltpu.make_async_remote_copy(
            src_ref=source,
            dst_ref=target,
            send_sem=left,
            recv_sem=got,
            device_id=device,
            device_id_type=MESH,
        ).start()

    def awaiting(ref, semaphore):
        return pltpu.make_async_remote_copy(
            src_ref=ref,
            dst_ref=ref,
            send_sem=semaphore,
            recv_sem=semaphore,
            device_id={"row": row_peer(1)},
            device_id_type=MESH,
        )

    def arrive(ref, semaphore):
        awaiting(ref, semaphore).wait_recv()

    has_right, has_left = me < n_row - 1, me > 0
    edge = jnp.logical_or(me == 0, me == n_row - 1)

    def greet(semaphore):
        for name, spot, size in (("col", col, n_col), ("samp", samp, n_samp), ("job", job, p_job)):
            for k in range(1, size):
                device = {name: lax.rem(spot + k, size)}
                pl.semaphore_signal(semaphore, inc=1, device_id=device, device_id_type=MESH)

        @pl.when(has_right)
        def _():
            device = {"row": jnp.minimum(me + 1, n_row - 1)}
            pl.semaphore_signal(semaphore, inc=1, device_id=device, device_id_type=MESH)

        @pl.when(has_left)
        def _():
            device = {"row": jnp.maximum(me - 1, 0)}
            pl.semaphore_signal(semaphore, inc=1, device_id=device, device_id_type=MESH)

    def await_greetings(semaphore):
        others = (n_col - 1) + (n_samp - 1) + (p_job - 1)
        pl.semaphore_wait(semaphore, others + jnp.where(edge, 1, 2))

    rounds = greeting.shape[0]
    barrier = pltpu.get_barrier_semaphore()
    greet(barrier)

    loads = {}
    for index, (name, source, target) in enumerate(
        (
            ("asym", asym_hbm, asym),
            ("pair", pair_hbm, pair),
            ("rel", rel_hbm, rel),
            ("pair_gain", pair_gain_hbm, pair_gain),
            ("bias_weight", bias_weight_hbm, bias_weight),
            ("qkv", qkv_hbm.at[0], qkv),
            ("token_gain", token_gain_hbm, token_gain),
            ("ow", out_weight_hbm.at[0], ow.at[me]),
            ("valid", valid_hbm, valid),
        )
    ):
        loads[name] = pltpu.make_async_copy(source, target, local_sem.at[index])
    loads["tok"] = pltpu.make_async_copy(tokens_hbm, own, local_sem.at[9])
    for name in ("tok", "token_gain", "asym", "pair", "rel", "pair_gain", "bias_weight", "qkv", "ow", "valid"):
        loads[name].start()

    def ow_piece(source, a, b):
        first = aligned(lax.rem(job + a, n_job) * piece_rows if p_job > 1 else 0, piece_rows)
        start = aligned(lax.rem(col + b, n_col) * piece_cols if p_col > 1 else 0, piece_cols)
        return ow.at[source, pl.ds(first, piece_rows), pl.ds(start, piece_cols)]

    chips = [(a, b) for a in range(p_job) for b in range(p_col)]

    def send_ow():
        for k in range(1, n_row):
            send(ow_piece(me, 0, 0), ow_piece(me, 0, 0), sent.at[2], ow_got.at[0, k - 1], {"row": row_peer(k)})

    def pair_ow(k, a, b):
        piece = ow_piece(row_source(k), a, b)
        for e in range(1, n_samp):
            device = {"samp": lax.rem(samp + e, n_samp)}
            send(piece, piece, ow_sent.at[e - 1], ow_got.at[2, k - 1], device)

    def spread_ow(k):
        piece = ow_piece(row_source(k), 0, 0)
        arrive(piece, ow_got.at[0, k - 1])
        for a, b in chips[1:]:
            device = {
                name: lax.rem(spot + step, size)
                for name, spot, step, size in (("job", job, a, n_job), ("col", col, b, n_col))
                if step
            }
            send(piece, piece, sent.at[2], ow_got.at[1, k - 1], device)
        pair_ow(k, 0, 0)

    def collect_ow(k):
        if pieces > 1:
            arrive(ow.at[row_source(k), pl.ds(0, out_rows - out_rows // pieces)], ow_got.at[1, k - 1])
            for a, b in chips[1:]:
                pair_ow(k, a, b)

    def take_ow(k):
        arrive(ow.at[row_source(k)], ow_got.at[2, k - 1])

    low = 2 * me < n_row
    outward = jnp.where(low, -1, 1)
    near = jnp.minimum(me, n_row - 1 - me)

    def nearest(j):
        step = (j + 1) // 2
        both = jnp.where(low == (j % 2 == 1), -step, step)
        one = jnp.where(low, j - near, near - j)
        return me + jnp.where(j <= 2 * near, both, one)

    def push_tokens(s, source, way):
        target = me + way

        @pl.when(jnp.logical_and(target >= 0, target < n_row))
        def _():
            send(
                tok.at[s, source],
                tok.at[s, source],
                tok_sent.at[(way + 1) // 2, source],
                tok_got.at[s, source],
                {"row": jnp.clip(target, 0, n_row - 1)},
            )

    def send_tokens(s):
        push_tokens(s, me, -outward)
        push_tokens(s, me, outward)

    def take_tokens(s, distance):
        for way in (outward, -outward):
            source = me + way * distance

            @pl.when(jnp.logical_and(source >= 0, source < n_row))
            def _():
                place = jnp.clip(source, 0, n_row - 1)
                arrive(tok.at[s, place], tok_got.at[s, place])
                push_tokens(s, place, -way)

    def bias_part(target):
        return bias_send.at[
            pl.ds(pl.multiple_of(target * part_rows, part_rows), part_rows)
        ]

    def spread_bias(k):
        place = bias_recv.at[row_source(k) * n_plane + plane]
        held = place if k else bias_part(me)
        for m in range(1, n_plane):
            other = lax.rem(plane + m, n_plane)
            send(
                held,
                place,
                sent.at[1],
                bias_got.at[n_row - 1],
                {"col": lax.div(other, n_samp), "samp": lax.rem(other, n_samp)},
            )

    def send_bias():
        for k in range(1, n_row):
            target = row_peer(k)
            send(
                bias_part(target),
                bias_recv.at[me * n_plane + plane],
                sent.at[1],
                bias_got.at[k - 1],
                {"row": target},
            )
        spread_bias(0)

    def pass_bias(k):
        arrive(bias_recv.at[row_source(k) * n_plane + plane], bias_got.at[k - 1])
        spread_bias(k)

    def take_bias():
        if n_plane > 1:
            arrive(bias_recv.at[pl.ds(0, n_row * (n_plane - 1))], bias_got.at[n_row - 1])

    own_bias = pltpu.make_async_copy(
        bias_part(me), bias_recv.at[me * n_plane + plane], local_sem.at[11]
    )

    head_of_lane = lax.broadcasted_iota(jnp.int32, (total, local_width), 1)
    head_masks = [
        jnp.logical_and(head_of_lane >= h * HEAD_DIM, head_of_lane < (h + 1) * HEAD_DIM)
        for h in range(local_heads)
    ]
    scale = 1.0 / math.sqrt(HEAD_DIM)

    def project(sources, chosen=slice(None)):
        normed = tok[chosen, sources].reshape(-1, width)
        for index, target in enumerate((query, key, value)):
            done = lax.dot_general(
                normed, qkv[index], (((1,), (1,)), ((), ())), preferred_element_type=jnp.float32
            ).astype(jnp.bfloat16)
            target[chosen, sources] = done.reshape(target[chosen, sources].shape)

    def attend(s):
        whole = (total, local_width)
        keys = key[s].reshape(whole).astype(jnp.float32)
        values = value[s].reshape(whole).astype(jnp.float32)
        keys = jnp.concatenate(
            [jnp.where(mask, keys, 0.0).astype(jnp.bfloat16) for mask in head_masks], axis=0
        )
        values = jnp.concatenate(
            [jnp.where(mask, values, 0.0).astype(jnp.bfloat16) for mask in head_masks], axis=0
        )
        scores = lax.dot_general(
            query[s].reshape(whole), keys, (((1,), (1,)), ((), ())), preferred_element_type=jnp.float32
        )
        probs = []
        for h in range(local_heads):
            span = slice(h * total, (h + 1) * total)
            logits = scores[:, span] * scale + bias[:, span]
            weights = jnp.exp(logits - jnp.max(logits, axis=-1, keepdims=True))
            inverse = 1.0 / jnp.sum(weights, axis=-1, keepdims=True)
            probs.append((weights * inverse).astype(jnp.bfloat16))
        mixed = jnp.dot(
            jnp.concatenate(probs, axis=1), values, preferred_element_type=jnp.float32
        ).astype(jnp.bfloat16)
        attended[s] = mixed.reshape(n_row, token_rows, local_width)

    def give(first, last):
        for j in range(n_row - 1, 0, -1):
            target = nearest(j)
            for s in range(first, last):
                send(
                    attended.at[s, target],
                    heads_in.at[me * samples + s],
                    sent.at[0],
                    att_got.at[me],
                    {"row": target},
                )
        for s in range(first, last):
            heads_in[me * samples + s] = attended[s, me]

    def take_attended(source):
        arrive(heads_in.at[pl.ds(source * samples, samples)], att_got.at[source])

    def build_bias():
        lanes_at = lax.broadcasted_iota(jnp.int32, (part_rows, LANES), 1)
        for tile in range(total // LANES):
            padded = lanes_at[:stripes] + tile * LANES >= valid[0]
            for r in range(n_row):
                parts = [bias_recv[r * n_plane + tile * fold + m] for m in range(fold)]
                for q in range(fold):
                    whole = None
                    for m in range(fold):
                        shift = ((m - q) % fold) * tile_cols
                        turned = pltpu.roll(parts[m], shift, 1) if shift else parts[m]
                        whole = (
                            turned
                            if whole is None
                            else jnp.where(lanes_at >= m * tile_cols, turned, whole)
                        )
                    at = r * tile_rows + q * stripes
                    for h in range(local_heads):
                        bias[
                            at : at + stripes,
                            h * total + tile * LANES : h * total + (tile + 1) * LANES,
                        ] = jnp.where(padded, -1e30, whole[h * stripes : (h + 1) * stripes])

    everything = slice(None)
    with mark("tokload"):
        loads["tok"].wait()
        loads["token_gain"].wait()
    with mark("norm"):
        rows = own[...].reshape(samples * token_rows, width).astype(jnp.float32)
        normed = normalize(rows, token_gain[...]).astype(jnp.bfloat16)
        tok[:, me] = normed.reshape(samples, token_rows, width)
    with mark("barrier"):
        await_greetings(barrier)

    early = min(2, samples)
    for s in range(early):
        send_tokens(s)

    @pl.when(jnp.logical_not(relay))
    def _():
        for s in range(early, samples):
            send_tokens(s)

    with mark("pairload"):
        for name in ("asym", "pair", "rel", "pair_gain", "bias_weight"):
            loads[name].wait()
    first_row, first_col = me * tile_rows, plane * tile_cols
    sub = lax.broadcasted_iota(jnp.int32, (tile_cols, LANES), 0)
    lane = lax.broadcasted_iota(jnp.int32, (tile_cols, LANES), 1)
    with mark("pairprep"):
        col_chain = jnp.zeros((tile_cols, LANES), jnp.int32)
        for j in range(tile_cols):
            col_chain = jnp.where(sub == j, asym[first_col + j], col_chain)
        reach = bins // 2 - 1
        turned_weight = bias_weight[...]
    def pair_stripes(first, last):
        for t in range(first, last):
            hots, rows = [], []
            for q in range(fold):
                i = q * stripes + t
                offset = jnp.clip(first_row + i - first_col - sub, -reach, reach) + reach
                bin_ids = jnp.where(col_chain == asym[first_row + i], offset, bins - 1)
                hots.append(jnp.where(bin_ids == lane, 1.0, 0.0).astype(jnp.bfloat16))
                rows.append(pair[i].astype(jnp.float32))
            summed = jnp.concatenate(rows, axis=0) + jnp.dot(
                jnp.concatenate(hots, axis=0), rel[...], preferred_element_type=jnp.float32
            )
            normed_pair = normalize(summed, pair_gain[...]).astype(jnp.bfloat16)
            projected = lax.dot_general(
                turned_weight, normed_pair, (((1,), (1,)), ((), ())), preferred_element_type=jnp.float32
            )
            bias_send[pl.ds(t, all_heads, stride=stripes), :] = projected

    for r in range(rounds):
        greet(greeting.at[r])
        with mark("pair"):
            pair_stripes(r * stripes // rounds, (r + 1) * stripes // rounds)
        with mark("greeting"):
            await_greetings(greeting.at[r])

    with mark("loads"):
        for name in ("ow", "qkv", "valid"):
            loads[name].wait()
    send_bias()
    own_bias.start()

    @pl.when(relay)
    def _():
        send_ow()
        for s in range(early, samples):
            send_tokens(s)

    @pl.when(edge)
    def _():
        with mark("project"):
            project(me)

    def step(distance):
        for s in range(early if distance == 1 else 0, samples):
            with mark("tokens"):
                take_tokens(s, distance)
            if distance == 1 and s == min(3, samples - 1):

                @pl.when(relay)
                def _():
                    with mark("ow0"):
                        for k in range(1, n_row):
                            spread_ow(k)

        @pl.when(edge)
        def _():
            with mark("project"):
                project(jnp.where(me == 0, distance, me - distance))

    def first_bias():
        with mark("bias0"):
            for k in range(1, n_row):
                pass_bias(k)

    if n_row > 2:
        with mark("tokens0"):
            for s in range(early):
                take_tokens(s, 1)

    @pl.when(relay)
    def _():
        first_bias()

    if n_row > 2:
        step(1)

    @pl.when(jnp.logical_not(relay))
    def _():
        first_bias()

    for distance in range(2, n_row - 1):
        step(distance)

    def relay_ow():
        @pl.when(relay)
        def _():
            with mark("ow1"):
                for k in range(1, n_row):
                    collect_ow(k)

    def prepare_bias():
        with mark("bias2"):
            own_bias.wait()
            take_bias()
        with mark("build"):
            build_bias()

    def finish_samples(first, last):
        with mark("attend"):
            for s in range(first, last):
                attend(s)
        with mark("give"):
            give(first, last)

    batch = max(samples // 2, 1)
    batches = [(first, min(first + batch, samples)) for first in range(0, samples, batch)]

    @pl.when(edge)
    def _():
        prepare_bias()
        for first, last in batches:
            with mark("tokense"):
                for s in range(first, last):
                    take_tokens(s, n_row - 1)
            with mark("project"):
                project(n_row - 1 - me, slice(first, last))
            finish_samples(first, last)
            if first == 0:
                relay_ow()

    @pl.when(jnp.logical_not(edge))
    def _():
        for s in range(samples):
            with mark("tokensi"):
                take_tokens(s, n_row - 1)
        with mark("projecti"):
            project(slice(None))
        prepare_bias()
        for first, last in batches:
            finish_samples(first, last)
        relay_ow()

    @pl.when(jnp.logical_not(relay))
    def _():
        with mark("ow3"):
            for k in range(1, n_row):
                take_ow(k)

    def term(source):
        flat = heads_in[pl.ds(source * samples, samples)].reshape(samples * token_rows, local_width)
        return jnp.dot(flat, ow[source], preferred_element_type=jnp.float32)

    with mark("product0"):
        flat_shape = (samples * token_rows, width)
        total_sum[...] = own[...].reshape(flat_shape).astype(jnp.float32) + term(me)
    for j in range(1, n_row):
        source = nearest(j)
        with mark("attwait"):
            take_attended(source)
        with mark("product"):
            if j < n_row - 1:
                total_sum[...] += term(source)
            else:
                result = total_sum[...] + term(source)
                out[...] = result.astype(out.dtype).reshape(samples, token_rows, width)

    with mark("fin"):
        for source in range(n_row):
            for rightward in (True, False):

                @pl.when(jnp.logical_and(source <= me, has_right) if rightward else jnp.logical_and(source >= me, has_left))
                def _():
                    awaiting(tok.at[:, source], tok_sent.at[1 if rightward else 0, source]).wait_send()

        awaiting(bias_recv.at[pl.ds(0, n_row * n_plane - 1)], sent.at[1]).wait_send()
        awaiting(attended.at[:, pl.ds(0, n_row - 1)], sent.at[0]).wait_send()

        @pl.when(relay)
        def _():
            awaiting(ow.at[pl.ds(0, n_row - 1)], sent.at[2]).wait_send()
            for e in range(1, n_samp):
                awaiting(ow.at[pl.ds(0, n_row - 1)], ow_sent.at[e - 1]).wait_send()


def per_device(
    axes,
    pair_repr,
    asym_id,
    valid_len,
    rel_embed,
    pair_gain,
    bias_weight,
    tokens,
    token_gain,
    qkv_weight,
    out_weight,
):
    n_job, n_row, n_col, n_samp = axes
    samples, token_rows, width = tokens.shape
    total = n_row * token_rows
    n_plane = n_col * n_samp
    heads = bias_weight.shape[1]
    local_heads = heads // n_row
    tile_rows, tile_cols, channels = pair_repr.shape
    local_width = qkv_weight.shape[-1]
    out_rows = out_weight.shape[1]
    cuts = (1 if out_rows % (16 * n_job) else n_job, 1 if width % (LANES * n_col) else n_col)
    stripes = tile_rows // (LANES // tile_cols)
    part_rows = local_heads * stripes
    bf16, f32 = jnp.bfloat16, jnp.float32
    dma = pltpu.SemaphoreType.DMA
    any_spec = pl.BlockSpec(memory_space=pltpu.HBM)
    return pl.pallas_call(
        functools.partial(kernel, axes, cuts),
        out_shape=jax.ShapeDtypeStruct(tokens.shape, tokens.dtype),
        in_specs=[any_spec] * 10,
        out_specs=pl.BlockSpec(memory_space=pltpu.VMEM),
        scratch_shapes=[
            pltpu.SMEM(asym_id.shape, jnp.int32),
            pltpu.SMEM(valid_len.shape, jnp.int32),
            pltpu.VMEM(pair_repr.shape, bf16),
            pltpu.VMEM(rel_embed.shape, bf16),
            pltpu.VMEM((1, channels), f32),
            pltpu.VMEM(bias_weight.shape[::-1], bf16),
            pltpu.VMEM(token_gain.shape, f32),
            pltpu.VMEM((3, local_width, width), bf16),
            pltpu.VMEM(tokens.shape, bf16),
            pltpu.VMEM((samples, n_row, token_rows, width), bf16),
            pltpu.VMEM((n_row, out_rows, width), bf16),
            pltpu.VMEM((heads * stripes, LANES), f32),
            pltpu.VMEM((n_row * n_plane, part_rows, LANES), f32),
            pltpu.VMEM((total, local_heads * total), f32),
            pltpu.VMEM((samples, n_row, token_rows, local_width), bf16),
            pltpu.VMEM((samples, n_row, token_rows, local_width), bf16),
            pltpu.VMEM((samples, n_row, token_rows, local_width), bf16),
            pltpu.VMEM((samples, n_row, token_rows, local_width), bf16),
            pltpu.VMEM((n_row * samples, token_rows, local_width), bf16),
            pltpu.VMEM((samples * token_rows, width), f32),
            dma((12,)),
            dma((samples, n_row)),
            dma((2, n_row)),
            dma((n_row,)),
            dma((3, n_row - 1)),
            dma((max(n_samp - 1, 1),)),
            dma((n_row,)),
            dma((3,)),
            pltpu.SemaphoreType.REGULAR((max(n_row - 2, 2),)),
        ],
        compiler_params=pltpu.CompilerParams(
            collective_id=0, has_side_effects=True, vmem_limit_bytes=24 * 1024 * 1024
        ),
    )(
        *(
            operand if operand is valid_len else pltpu.with_memory_space_constraint(operand, pltpu.HBM)
            for operand in (
                asym_id,
                valid_len,
                pair_repr,
                rel_embed,
                pair_gain.reshape(1, channels),
                bias_weight.T,
                tokens,
                token_gain,
                jnp.swapaxes(qkv_weight, 2, 3),
                out_weight,
            )
        )
    )


def solution(mesh):
    axes = tuple(mesh.shape[name] for name in ("job", "row", "col", "samp"))
    return jax.shard_map(
        functools.partial(per_device, axes),
        mesh=mesh,
        in_specs=(
            P(("job", "row"), ("col", "samp"), None),
            P("job"),
            P("job"),
            P(),
            P(),
            P(),
            P(("job", "col", "samp"), "row", None),
            P(),
            P(None, None, None, "row"),
            P(None, "row", None),
        ),
        out_specs=P(("job", "col", "samp"), "row", None),
        check_vma=False,
    )
```

```python
import contextlib
import functools
import math

import jax
import jax.numpy as jnp
from jax import lax
from jax.experimental import pallas as pl
from jax.experimental.pallas import tpu as pltpu
from jax.sharding import PartitionSpec as P

HEAD_DIM = 48
EPSILON = 1e-05
LANES = 128
MESH = pl.DeviceIdType.MESH
mark = contextlib.nullcontext


def normalize(values, gain_vector):
    average = jnp.mean(values, axis=-1, keepdims=True)
    centered = values - average
    variance = jnp.mean(centered * centered, axis=-1, keepdims=True)
    return centered * lax.rsqrt(variance + EPSILON) * gain_vector


def back(position, shift, size):
    return lax.rem(position + (size - shift), size) if shift else position


def aligned(value, unit):
    return value if isinstance(value, int) else pl.multiple_of(value, unit)


def kernel(
    axes,
    cuts,
    asym_hbm,
    valid_hbm,
    pair_hbm,
    rel_hbm,
    pair_gain_hbm,
    bias_weight_hbm,
    tokens_hbm,
    token_gain_hbm,
    qkv_hbm,
    out_weight_hbm,
    out,
    asym,
    valid,
    pair,
    rel,
    pair_gain,
    bias_weight,
    token_gain,
    qkv,
    own,
    tok,
    ow,
    bias_send,
    bias_recv,
    bias,
    query,
    key,
    value,
    attended,
    heads_in,
    total_sum,
    local_sem,
    tok_got,
    tok_sent,
    bias_got,
    ow_got,
    ow_sent,
    att_got,
    sent,
    greeting,
):
    n_job, n_row, n_col, n_samp = axes
    job, me = lax.axis_index("job"), lax.axis_index("row")
    col, samp = lax.axis_index("col"), lax.axis_index("samp")
    samples, token_rows, width = tokens_hbm.shape
    total = n_row * token_rows
    tile_rows, tile_cols, channels = pair.shape
    bins = rel.shape[0]
    plane = col * n_samp + samp
    all_heads = bias_weight.shape[0]
    local_heads = all_heads // n_row
    local_width = local_heads * HEAD_DIM
    fold = LANES // tile_cols
    stripes = tile_rows // fold
    part_rows = bias_recv.shape[1]
    out_rows = ow.shape[1]
    n_plane = n_col * n_samp
    p_job, p_col = cuts
    pieces = p_job * p_col
    piece_rows, piece_cols = out_rows // p_job, width // p_col
    relay = samp == n_samp - 1

    def row_peer(k):
        return lax.rem(me + k, n_row)

    def row_source(k):
        return back(me, k, n_row)

    def send(source, target, left, got, device):
        pltpu.make_async_remote_copy(
            src_ref=source,
            dst_ref=target,
            send_sem=left,
            recv_sem=got,
            device_id=device,
            device_id_type=MESH,
        ).start()

    def awaiting(ref, semaphore):
        return pltpu.make_async_remote_copy(
            src_ref=ref,
            dst_ref=ref,
            send_sem=semaphore,
            recv_sem=semaphore,
            device_id={"row": row_peer(1)},
            device_id_type=MESH,
        )

    def arrive(ref, semaphore):
        awaiting(ref, semaphore).wait_recv()

    has_right, has_left = me < n_row - 1, me > 0
    edge = jnp.logical_or(me == 0, me == n_row - 1)

    def greet(semaphore):
        for name, spot, size in (("col", col, n_col), ("samp", samp, n_samp), ("job", job, p_job)):
            for k in range(1, size):
                device = {name: lax.rem(spot + k, size)}
                pl.semaphore_signal(semaphore, inc=1, device_id=device, device_id_type=MESH)

        @pl.when(has_right)
        def _():
            device = {"row": jnp.minimum(me + 1, n_row - 1)}
            pl.semaphore_signal(semaphore, inc=1, device_id=device, device_id_type=MESH)

        @pl.when(has_left)
        def _():
            device = {"row": jnp.maximum(me - 1, 0)}
            pl.semaphore_signal(semaphore, inc=1, device_id=device, device_id_type=MESH)

    def await_greetings(semaphore):
        others = (n_col - 1) + (n_samp - 1) + (p_job - 1)
        pl.semaphore_wait(semaphore, others + jnp.where(edge, 1, 2))

    rounds = greeting.shape[0]
    barrier = pltpu.get_barrier_semaphore()
    greet(barrier)

    loads = {}
    for index, (name, source, target) in enumerate(
        (
            ("asym", asym_hbm, asym),
            ("pair", pair_hbm, pair),
            ("rel", rel_hbm, rel),
            ("pair_gain", pair_gain_hbm, pair_gain),
            ("bias_weight", bias_weight_hbm, bias_weight),
            ("qkv", qkv_hbm.at[0], qkv),
            ("token_gain", token_gain_hbm, token_gain),
            ("ow", out_weight_hbm.at[0], ow.at[me]),
            ("valid", valid_hbm, valid),
        )
    ):
        loads[name] = pltpu.make_async_copy(source, target, local_sem.at[index])
    loads["tok"] = pltpu.make_async_copy(tokens_hbm, own, local_sem.at[9])
    for name in ("tok", "token_gain", "asym", "pair", "rel", "pair_gain", "bias_weight", "qkv", "ow", "valid"):
        loads[name].start()

    def ow_piece(source, a, b):
        first = aligned(lax.rem(job + a, n_job) * piece_rows if p_job > 1 else 0, piece_rows)
        start = aligned(lax.rem(col + b, n_col) * piece_cols if p_col > 1 else 0, piece_cols)
        return ow.at[source, pl.ds(first, piece_rows), pl.ds(start, piece_cols)]

    chips = [(a, b) for a in range(p_job) for b in range(p_col)]

    def send_ow():
        for k in range(1, n_row):
            send(ow_piece(me, 0, 0), ow_piece(me, 0, 0), sent.at[2], ow_got.at[k - 1], {"row": row_peer(k)})

    def pair_ow(k, a, b):
        piece = ow_piece(row_source(k), a, b)
        for e in range(1, n_samp):
            device = {"samp": lax.rem(samp + e, n_samp)}
            send(piece, piece, ow_sent.at[e - 1], ow_got.at[n_row], device)

    def spread_ow(k):
        piece = ow_piece(row_source(k), 0, 0)
        arrive(piece, ow_got.at[k - 1])
        for a, b in chips[1:]:
            device = {
                name: lax.rem(spot + step, size)
                for name, spot, step, size in (("job", job, a, n_job), ("col", col, b, n_col))
                if step
            }
            send(piece, piece, sent.at[2], ow_got.at[n_row - 1], device)
        pair_ow(k, 0, 0)

    def collect_ow():
        if pieces > 1:
            others = ow.at[pl.ds(0, n_row - 1), pl.ds(0, out_rows - out_rows // pieces)]
            arrive(others, ow_got.at[n_row - 1])
            for k in range(1, n_row):
                for a, b in chips[1:]:
                    pair_ow(k, a, b)

    def take_ow():
        arrive(ow.at[pl.ds(0, n_row - 1)], ow_got.at[n_row])

    low = 2 * me < n_row
    outward = jnp.where(low, -1, 1)
    near = jnp.minimum(me, n_row - 1 - me)

    def nearest(j):
        step = (j + 1) // 2
        both = jnp.where(low == (j % 2 == 1), -step, step)
        one = jnp.where(low, j - near, near - j)
        return me + jnp.where(j <= 2 * near, both, one)

    def push_tokens(s, source, way):
        target = me + way

        @pl.when(jnp.logical_and(target >= 0, target < n_row))
        def _():
            send(
                tok.at[s, source],
                tok.at[s, source],
                tok_sent.at[(way + 1) // 2],
                tok_got.at[s, source],
                {"row": jnp.clip(target, 0, n_row - 1)},
            )

    def send_tokens(s):
        push_tokens(s, me, -outward)
        push_tokens(s, me, outward)

    def take_tokens(s, distance):
        for way in (outward, -outward):
            source = me + way * distance

            @pl.when(jnp.logical_and(source >= 0, source < n_row))
            def _():
                place = jnp.clip(source, 0, n_row - 1)
                arrive(tok.at[s, place], tok_got.at[s, place])
                push_tokens(s, place, -way)

    def bias_part(target):
        return bias_send.at[
            pl.ds(pl.multiple_of(target * part_rows, part_rows), part_rows)
        ]

    def spread_bias(k):
        place = bias_recv.at[row_source(k) * n_plane + plane]
        held = place if k else bias_part(me)
        for m in range(1, n_plane):
            other = lax.rem(plane + m, n_plane)
            send(
                held,
                place,
                sent.at[1],
                bias_got.at[n_row - 1],
                {"col": lax.div(other, n_samp), "samp": lax.rem(other, n_samp)},
            )

    def send_bias():
        for k in range(1, n_row):
            target = row_peer(k)
            send(
                bias_part(target),
                bias_recv.at[me * n_plane + plane],
                sent.at[1],
                bias_got.at[k - 1],
                {"row": target},
            )
        spread_bias(0)

    def pass_bias(k):
        arrive(bias_recv.at[row_source(k) * n_plane + plane], bias_got.at[k - 1])
        spread_bias(k)

    def take_bias():
        if n_plane > 1:
            arrive(bias_recv.at[pl.ds(0, n_row * (n_plane - 1))], bias_got.at[n_row - 1])

    own_bias = pltpu.make_async_copy(
        bias_part(me), bias_recv.at[me * n_plane + plane], local_sem.at[10]
    )

    head_of_lane = lax.broadcasted_iota(jnp.int32, (total, local_width), 1)
    head_masks = [
        jnp.logical_and(head_of_lane >= h * HEAD_DIM, head_of_lane < (h + 1) * HEAD_DIM)
        for h in range(local_heads)
    ]
    scale = 1.0 / math.sqrt(HEAD_DIM)

    def project(sources, chosen=slice(None)):
        normed = tok[chosen, sources].reshape(-1, width)
        for index, target in enumerate((query, key, value)):
            done = lax.dot_general(
                normed, qkv[index], (((1,), (1,)), ((), ())), preferred_element_type=jnp.float32
            ).astype(jnp.bfloat16)
            target[chosen, sources] = done.reshape(target[chosen, sources].shape)

    def attend(s):
        whole = (total, local_width)
        keys = key[s].reshape(whole).astype(jnp.float32)
        values = value[s].reshape(whole).astype(jnp.float32)
        keys = jnp.concatenate(
            [jnp.where(mask, keys, 0.0).astype(jnp.bfloat16) for mask in head_masks], axis=0
        )
        values = jnp.concatenate(
            [jnp.where(mask, values, 0.0).astype(jnp.bfloat16) for mask in head_masks], axis=0
        )
        scores = lax.dot_general(
            query[s].reshape(whole), keys, (((1,), (1,)), ((), ())), preferred_element_type=jnp.float32
        )
        probs = []
        for h in range(local_heads):
            span = slice(h * total, (h + 1) * total)
            logits = scores[:, span] * scale + bias[:, span]
            weights = jnp.exp(logits - jnp.max(logits, axis=-1, keepdims=True))
            inverse = 1.0 / jnp.sum(weights, axis=-1, keepdims=True)
            probs.append((weights * inverse).astype(jnp.bfloat16))
        mixed = jnp.dot(
            jnp.concatenate(probs, axis=1), values, preferred_element_type=jnp.float32
        ).astype(jnp.bfloat16)
        attended[s] = mixed.reshape(n_row, token_rows, local_width)

    def give(first, last):
        for j in range(n_row - 1, 0, -1):
            target = nearest(j)
            for s in range(first, last):
                send(
                    attended.at[s, target],
                    heads_in.at[me * samples + s],
                    sent.at[0],
                    att_got.at[me],
                    {"row": target},
                )
        for s in range(first, last):
            heads_in[me * samples + s] = attended[s, me]

    def take_attended(source):
        arrive(heads_in.at[pl.ds(source * samples, samples)], att_got.at[source])

    def build_bias():
        lanes_at = lax.broadcasted_iota(jnp.int32, (part_rows, LANES), 1)
        for tile in range(total // LANES):
            padded = lanes_at[:stripes] + tile * LANES >= valid[0]
            for r in range(n_row):
                parts = [bias_recv[r * n_plane + tile * fold + m] for m in range(fold)]
                for q in range(fold):
                    whole = None
                    for m in range(fold):
                        shift = ((m - q) % fold) * tile_cols
                        turned = pltpu.roll(parts[m], shift, 1) if shift else parts[m]
                        whole = (
                            turned
                            if whole is None
                            else jnp.where(lanes_at >= m * tile_cols, turned, whole)
                        )
                    at = r * tile_rows + q * stripes
                    for h in range(local_heads):
                        bias[
                            at : at + stripes,
                            h * total + tile * LANES : h * total + (tile + 1) * LANES,
                        ] = jnp.where(padded, -1e30, whole[h * stripes : (h + 1) * stripes])

    everything = slice(None)
    with mark("tokload"):
        loads["tok"].wait()
        loads["token_gain"].wait()
    with mark("norm"):
        rows = own[...].reshape(samples * token_rows, width).astype(jnp.float32)
        normed = normalize(rows, token_gain[...]).astype(jnp.bfloat16)
        tok[:, me] = normed.reshape(samples, token_rows, width)
    with mark("barrier"):
        await_greetings(barrier)

    early = min(2, samples)
    for s in range(early):
        send_tokens(s)

    @pl.when(jnp.logical_not(relay))
    def _():
        for s in range(early, samples):
            send_tokens(s)

    with mark("pairload"):
        for name in ("asym", "pair", "rel", "pair_gain", "bias_weight"):
            loads[name].wait()
    first_row, first_col = me * tile_rows, plane * tile_cols
    sub = lax.broadcasted_iota(jnp.int32, (tile_cols, LANES), 0)
    lane = lax.broadcasted_iota(jnp.int32, (tile_cols, LANES), 1)
    with mark("pairprep"):
        col_chain = jnp.zeros((tile_cols, LANES), jnp.int32)
        for j in range(tile_cols):
            col_chain = jnp.where(sub == j, asym[first_col + j], col_chain)
        reach = bins // 2 - 1
        turned_weight = bias_weight[...]
    def pair_stripes(first, last):
        for t in range(first, last):
            hots, rows = [], []
            for q in range(fold):
                i = q * stripes + t
                offset = jnp.clip(first_row + i - first_col - sub, -reach, reach) + reach
                bin_ids = jnp.where(col_chain == asym[first_row + i], offset, bins - 1)
                hots.append(jnp.where(bin_ids == lane, 1.0, 0.0).astype(jnp.bfloat16))
                rows.append(pair[i].astype(jnp.float32))
            summed = jnp.concatenate(rows, axis=0) + jnp.dot(
                jnp.concatenate(hots, axis=0), rel[...], preferred_element_type=jnp.float32
            )
            normed_pair = normalize(summed, pair_gain[...]).astype(jnp.bfloat16)
            projected = lax.dot_general(
                turned_weight, normed_pair, (((1,), (1,)), ((), ())), preferred_element_type=jnp.float32
            )
            bias_send[pl.ds(t, all_heads, stride=stripes), :] = projected

    for r in range(rounds):
        greet(greeting.at[r])
        with mark("pair"):
            pair_stripes(r * stripes // rounds, (r + 1) * stripes // rounds)
        with mark("greeting"):
            await_greetings(greeting.at[r])

    with mark("loads"):
        for name in ("ow", "qkv", "valid"):
            loads[name].wait()
    send_bias()
    own_bias.start()

    @pl.when(relay)
    def _():
        send_ow()
        for s in range(early, samples):
            send_tokens(s)

    @pl.when(edge)
    def _():
        with mark("project"):
            project(me)

    def step(distance):
        for s in range(early if distance == 1 else 0, samples):
            with mark("tokens"):
                take_tokens(s, distance)
            if distance == 1 and s == min(3, samples - 1):

                @pl.when(relay)
                def _():
                    with mark("ow0"):
                        for k in range(1, n_row):
                            spread_ow(k)

        @pl.when(edge)
        def _():
            with mark("project"):
                project(jnp.where(me == 0, distance, me - distance))

    def first_bias():
        with mark("bias0"):
            for k in range(1, n_row):
                pass_bias(k)

    if n_row > 2:
        with mark("tokens0"):
            for s in range(early):
                take_tokens(s, 1)

    @pl.when(relay)
    def _():
        first_bias()

    if n_row > 2:
        step(1)

    @pl.when(jnp.logical_not(relay))
    def _():
        first_bias()

    for distance in range(2, n_row - 1):
        step(distance)

    def relay_ow():
        @pl.when(relay)
        def _():
            with mark("ow1"):
                collect_ow()

    def prepare_bias():
        with mark("bias2"):
            own_bias.wait()
            take_bias()
        with mark("build"):
            build_bias()

    def finish_samples(first, last):
        with mark("attend"):
            for s in range(first, last):
                attend(s)
        with mark("give"):
            give(first, last)

    batch = max(samples // 2, 1)
    batches = [(first, min(first + batch, samples)) for first in range(0, samples, batch)]

    @pl.when(edge)
    def _():
        prepare_bias()
        for first, last in batches:
            with mark("tokense"):
                for s in range(first, last):
                    take_tokens(s, n_row - 1)
            with mark("project"):
                project(n_row - 1 - me, slice(first, last))
            finish_samples(first, last)
        relay_ow()

    @pl.when(jnp.logical_not(edge))
    def _():
        for s in range(samples):
            with mark("tokensi"):
                take_tokens(s, n_row - 1)
        with mark("projecti"):
            project(slice(None))
        prepare_bias()
        for first, last in batches:
            finish_samples(first, last)
        relay_ow()

    @pl.when(jnp.logical_not(relay))
    def _():
        with mark("ow3"):
            take_ow()

    def term(source):
        flat = heads_in[pl.ds(source * samples, samples)].reshape(samples * token_rows, local_width)
        return jnp.dot(flat, ow[source], preferred_element_type=jnp.float32)

    with mark("product0"):
        flat_shape = (samples * token_rows, width)
        total_sum[...] = own[...].reshape(flat_shape).astype(jnp.float32) + term(me)
    for j in range(1, n_row):
        source = nearest(j)
        with mark("attwait"):
            take_attended(source)
        with mark("product"):
            if j < n_row - 1:
                total_sum[...] += term(source)
            else:
                result = total_sum[...] + term(source)
                out[...] = result.astype(out.dtype).reshape(samples, token_rows, width)

    with mark("fin"):
        for row in range(n_row):

            @pl.when(me == row)
            def _():
                if row < n_row - 1:
                    awaiting(tok.at[:, pl.ds(0, row + 1)], tok_sent.at[1]).wait_send()
                if row > 0:
                    awaiting(tok.at[:, pl.ds(0, n_row - row)], tok_sent.at[0]).wait_send()

        awaiting(bias_recv.at[pl.ds(0, n_row * n_plane - 1)], sent.at[1]).wait_send()
        awaiting(attended.at[:, pl.ds(0, n_row - 1)], sent.at[0]).wait_send()

        @pl.when(relay)
        def _():
            awaiting(ow.at[pl.ds(0, n_row - 1)], sent.at[2]).wait_send()
            for e in range(1, n_samp):
                awaiting(ow.at[pl.ds(0, n_row - 1)], ow_sent.at[e - 1]).wait_send()


def per_device(
    axes,
    pair_repr,
    asym_id,
    valid_len,
    rel_embed,
    pair_gain,
    bias_weight,
    tokens,
    token_gain,
    qkv_weight,
    out_weight,
):
    n_job, n_row, n_col, n_samp = axes
    samples, token_rows, width = tokens.shape
    total = n_row * token_rows
    n_plane = n_col * n_samp
    heads = bias_weight.shape[1]
    local_heads = heads // n_row
    tile_rows, tile_cols, channels = pair_repr.shape
    local_width = qkv_weight.shape[-1]
    out_rows = out_weight.shape[1]
    cuts = (1 if out_rows % (16 * n_job) else n_job, 1 if width % (LANES * n_col) else n_col)
    stripes = tile_rows // (LANES // tile_cols)
    part_rows = local_heads * stripes
    bf16, f32 = jnp.bfloat16, jnp.float32
    dma = pltpu.SemaphoreType.DMA
    any_spec = pl.BlockSpec(memory_space=pltpu.HBM)
    return pl.pallas_call(
        functools.partial(kernel, axes, cuts),
        out_shape=jax.ShapeDtypeStruct(tokens.shape, tokens.dtype),
        in_specs=[any_spec] * 10,
        out_specs=pl.BlockSpec(memory_space=pltpu.VMEM),
        scratch_shapes=[
            pltpu.SMEM(asym_id.shape, jnp.int32),
            pltpu.SMEM(valid_len.shape, jnp.int32),
            pltpu.VMEM(pair_repr.shape, bf16),
            pltpu.VMEM(rel_embed.shape, bf16),
            pltpu.VMEM((1, channels), f32),
            pltpu.VMEM(bias_weight.shape[::-1], bf16),
            pltpu.VMEM(token_gain.shape, f32),
            pltpu.VMEM((3, local_width, width), bf16),
            pltpu.VMEM(tokens.shape, bf16),
            pltpu.VMEM((samples, n_row, token_rows, width), bf16),
            pltpu.VMEM((n_row, out_rows, width), bf16),
            pltpu.VMEM((heads * stripes, LANES), f32),
            pltpu.VMEM((n_row * n_plane, part_rows, LANES), f32),
            pltpu.VMEM((total, local_heads * total), f32),
            pltpu.VMEM((samples, n_row, token_rows, local_width), bf16),
            pltpu.VMEM((samples, n_row, token_rows, local_width), bf16),
            pltpu.VMEM((samples, n_row, token_rows, local_width), bf16),
            pltpu.VMEM((samples, n_row, token_rows, local_width), bf16),
            pltpu.VMEM((n_row * samples, token_rows, local_width), bf16),
            pltpu.VMEM((samples * token_rows, width), f32),
            dma((11,)),
            dma((samples, n_row)),
            dma((2,)),
            dma((n_row,)),
            dma((n_row + 1,)),
            dma((max(n_samp - 1, 1),)),
            dma((n_row,)),
            dma((3,)),
            pltpu.SemaphoreType.REGULAR((max(n_row - 2, 2),)),
        ],
        compiler_params=pltpu.CompilerParams(
            collective_id=0, has_side_effects=True, vmem_limit_bytes=24 * 1024 * 1024
        ),
    )(
        *(
            operand if operand is valid_len else pltpu.with_memory_space_constraint(operand, pltpu.HBM)
            for operand in (
                asym_id,
                valid_len,
                pair_repr,
                rel_embed,
                pair_gain.reshape(1, channels),
                bias_weight.T,
                tokens,
                token_gain,
                jnp.swapaxes(qkv_weight, 2, 3),
                out_weight,
            )
        )
    )


def solution(mesh):
    axes = tuple(mesh.shape[name] for name in ("job", "row", "col", "samp"))
    return jax.shard_map(
        functools.partial(per_device, axes),
        mesh=mesh,
        in_specs=(
            P(("job", "row"), ("col", "samp"), None),
            P("job"),
            P("job"),
            P(),
            P(),
            P(),
            P(("job", "col", "samp"), "row", None),
            P(),
            P(None, None, None, "row"),
            P(None, "row", None),
        ),
        out_specs=P(("job", "col", "samp"), "row", None),
        check_vma=False,
    )
```

```python
import contextlib
import functools
import math

import jax
import jax.numpy as jnp
from jax import lax
from jax.experimental import pallas as pl
from jax.experimental.pallas import tpu as pltpu
from jax.sharding import PartitionSpec as P

HEAD_DIM = 48
EPSILON = 1e-05
LANES = 128
MESH = pl.DeviceIdType.MESH
mark = contextlib.nullcontext


def normalize(values, gain_vector):
    average = jnp.mean(values, axis=-1, keepdims=True)
    centered = values - average
    variance = jnp.mean(centered * centered, axis=-1, keepdims=True)
    return centered * lax.rsqrt(variance + EPSILON) * gain_vector


def back(position, shift, size):
    return lax.rem(position + (size - shift), size) if shift else position


def aligned(value, unit):
    return value if isinstance(value, int) else pl.multiple_of(value, unit)


def kernel(
    axes,
    cuts,
    asym_hbm,
    valid_hbm,
    pair_hbm,
    rel_hbm,
    pair_gain_hbm,
    bias_weight_hbm,
    tokens_hbm,
    token_gain_hbm,
    qkv_hbm,
    out_weight_hbm,
    out,
    asym,
    valid,
    pair,
    rel,
    pair_gain,
    bias_weight,
    token_gain,
    qkv,
    own,
    tok,
    ow,
    bias_send,
    bias_recv,
    bias,
    query,
    key,
    value,
    attended,
    heads_in,
    total_sum,
    local_sem,
    tok_got,
    tok_sent,
    bias_got,
    ow_got,
    ow_sent,
    att_got,
    sent,
    greeting,
):
    n_job, n_row, n_col, n_samp = axes
    job, me = lax.axis_index("job"), lax.axis_index("row")
    col, samp = lax.axis_index("col"), lax.axis_index("samp")
    samples, token_rows, width = tokens_hbm.shape
    total = n_row * token_rows
    tile_rows, tile_cols, channels = pair.shape
    bins = rel.shape[0]
    plane = col * n_samp + samp
    all_heads = bias_weight.shape[0]
    local_heads = all_heads // n_row
    local_width = local_heads * HEAD_DIM
    fold = LANES // tile_cols
    stripes = tile_rows // fold
    part_rows = bias_recv.shape[1]
    out_rows = ow.shape[1]
    n_plane = n_col * n_samp
    p_job, p_col = cuts
    pieces = p_job * p_col
    piece_rows, piece_cols = out_rows // p_job, width // p_col
    relay = samp == n_samp - 1

    def row_peer(k):
        return lax.rem(me + k, n_row)

    def row_source(k):
        return back(me, k, n_row)

    def send(source, target, left, got, device):
        pltpu.make_async_remote_copy(
            src_ref=source,
            dst_ref=target,
            send_sem=left,
            recv_sem=got,
            device_id=device,
            device_id_type=MESH,
        ).start()

    def awaiting(ref, semaphore):
        return pltpu.make_async_remote_copy(
            src_ref=ref,
            dst_ref=ref,
            send_sem=semaphore,
            recv_sem=semaphore,
            device_id={"row": row_peer(1)},
            device_id_type=MESH,
        )

    def arrive(ref, semaphore):
        awaiting(ref, semaphore).wait_recv()

    has_right, has_left = me < n_row - 1, me > 0
    edge = jnp.logical_or(me == 0, me == n_row - 1)

    def greet(semaphore):
        for name, spot, size in (("col", col, n_col), ("samp", samp, n_samp), ("job", job, p_job)):
            for k in range(1, size):
                device = {name: lax.rem(spot + k, size)}
                pl.semaphore_signal(semaphore, inc=1, device_id=device, device_id_type=MESH)

        @pl.when(has_right)
        def _():
            device = {"row": jnp.minimum(me + 1, n_row - 1)}
            pl.semaphore_signal(semaphore, inc=1, device_id=device, device_id_type=MESH)

        @pl.when(has_left)
        def _():
            device = {"row": jnp.maximum(me - 1, 0)}
            pl.semaphore_signal(semaphore, inc=1, device_id=device, device_id_type=MESH)

    def await_greetings(semaphore):
        others = (n_col - 1) + (n_samp - 1) + (p_job - 1)
        pl.semaphore_wait(semaphore, others + jnp.where(edge, 1, 2))

    rounds = greeting.shape[0]
    barrier = pltpu.get_barrier_semaphore()
    greet(barrier)

    loads = {}
    for index, (name, source, target) in enumerate(
        (
            ("asym", asym_hbm, asym),
            ("pair", pair_hbm, pair),
            ("rel", rel_hbm, rel),
            ("pair_gain", pair_gain_hbm, pair_gain),
            ("bias_weight", bias_weight_hbm, bias_weight),
            ("qkv", qkv_hbm.at[0], qkv),
            ("token_gain", token_gain_hbm, token_gain),
            ("ow", out_weight_hbm.at[0], ow.at[me]),
            ("valid", valid_hbm, valid),
        )
    ):
        loads[name] = pltpu.make_async_copy(source, target, local_sem.at[index])
    loads["tok"] = pltpu.make_async_copy(tokens_hbm, own, local_sem.at[9])
    for name in ("tok", "token_gain", "asym", "pair", "rel", "pair_gain", "bias_weight", "qkv", "ow", "valid"):
        loads[name].start()

    def ow_piece(source, a, b):
        first = aligned(lax.rem(job + a, n_job) * piece_rows if p_job > 1 else 0, piece_rows)
        start = aligned(lax.rem(col + b, n_col) * piece_cols if p_col > 1 else 0, piece_cols)
        return ow.at[source, pl.ds(first, piece_rows), pl.ds(start, piece_cols)]

    chips = [(a, b) for a in range(p_job) for b in range(p_col)]

    def send_ow():
        for k in range(1, n_row):
            send(ow_piece(me, 0, 0), ow_piece(me, 0, 0), sent.at[2], ow_got.at[k - 1], {"row": row_peer(k)})

    def pair_ow(k, a, b):
        piece = ow_piece(row_source(k), a, b)
        for e in range(1, n_samp):
            device = {"samp": lax.rem(samp + e, n_samp)}
            send(piece, piece, ow_sent.at[e - 1], ow_got.at[n_row], device)

    def spread_ow(k):
        piece = ow_piece(row_source(k), 0, 0)
        arrive(piece, ow_got.at[k - 1])
        for a, b in chips[1:]:
            device = {
                name: lax.rem(spot + step, size)
                for name, spot, step, size in (("job", job, a, n_job), ("col", col, b, n_col))
                if step
            }
            send(piece, piece, sent.at[2], ow_got.at[n_row - 1], device)
        pair_ow(k, 0, 0)

    def collect_ow():
        if pieces > 1:
            others = ow.at[pl.ds(0, n_row - 1), pl.ds(0, out_rows - out_rows // pieces)]
            arrive(others, ow_got.at[n_row - 1])
            for k in range(1, n_row):
                for a, b in chips[1:]:
                    pair_ow(k, a, b)

    def take_ow():
        arrive(ow.at[pl.ds(0, n_row - 1)], ow_got.at[n_row])

    low = 2 * me < n_row
    outward = jnp.where(low, -1, 1)
    near = jnp.minimum(me, n_row - 1 - me)

    def nearest(j):
        step = (j + 1) // 2
        both = jnp.where(low == (j % 2 == 1), -step, step)
        one = jnp.where(low, j - near, near - j)
        return me + jnp.where(j <= 2 * near, both, one)

    def push_tokens(s, source, way):
        target = me + way

        @pl.when(jnp.logical_and(target >= 0, target < n_row))
        def _():
            send(
                tok.at[s, source],
                tok.at[s, source],
                tok_sent.at[(way + 1) // 2],
                tok_got.at[s, source],
                {"row": jnp.clip(target, 0, n_row - 1)},
            )

    def send_tokens(s):
        push_tokens(s, me, -outward)
        push_tokens(s, me, outward)

    def take_tokens(s, distance):
        for way in (outward, -outward):
            source = me + way * distance

            @pl.when(jnp.logical_and(source >= 0, source < n_row))
            def _():
                place = jnp.clip(source, 0, n_row - 1)
                arrive(tok.at[s, place], tok_got.at[s, place])
                push_tokens(s, place, -way)

    def bias_part(target):
        return bias_send.at[
            pl.ds(pl.multiple_of(target * part_rows, part_rows), part_rows)
        ]

    def spread_bias(k):
        place = bias_recv.at[row_source(k) * n_plane + plane]
        held = place if k else bias_part(me)
        for m in range(1, n_plane):
            other = lax.rem(plane + m, n_plane)
            send(
                held,
                place,
                sent.at[1],
                bias_got.at[n_row - 1],
                {"col": lax.div(other, n_samp), "samp": lax.rem(other, n_samp)},
            )

    def send_bias():
        for k in range(1, n_row):
            target = row_peer(k)
            send(
                bias_part(target),
                bias_recv.at[me * n_plane + plane],
                sent.at[1],
                bias_got.at[k - 1],
                {"row": target},
            )
        spread_bias(0)

    def pass_bias(k):
        arrive(bias_recv.at[row_source(k) * n_plane + plane], bias_got.at[k - 1])
        spread_bias(k)

    def take_bias():
        if n_plane > 1:
            arrive(bias_recv.at[pl.ds(0, n_row * (n_plane - 1))], bias_got.at[n_row - 1])

    own_bias = pltpu.make_async_copy(
        bias_part(me), bias_recv.at[me * n_plane + plane], local_sem.at[10]
    )

    head_of_lane = lax.broadcasted_iota(jnp.int32, (total, local_width), 1)
    head_masks = [
        jnp.logical_and(head_of_lane >= h * HEAD_DIM, head_of_lane < (h + 1) * HEAD_DIM)
        for h in range(local_heads)
    ]
    scale = 1.0 / math.sqrt(HEAD_DIM)

    def project(sources, chosen=slice(None)):
        normed = tok[chosen, sources].reshape(-1, width)
        for index, target in enumerate((query, key, value)):
            done = lax.dot_general(
                normed, qkv[index], (((1,), (1,)), ((), ())), preferred_element_type=jnp.float32
            ).astype(jnp.bfloat16)
            target[chosen, sources] = done.reshape(target[chosen, sources].shape)

    def attend(s):
        whole = (total, local_width)
        keys = key[s].reshape(whole).astype(jnp.float32)
        values = value[s].reshape(whole).astype(jnp.float32)
        keys = jnp.concatenate(
            [jnp.where(mask, keys, 0.0).astype(jnp.bfloat16) for mask in head_masks], axis=0
        )
        values = jnp.concatenate(
            [jnp.where(mask, values, 0.0).astype(jnp.bfloat16) for mask in head_masks], axis=0
        )
        scores = lax.dot_general(
            query[s].reshape(whole), keys, (((1,), (1,)), ((), ())), preferred_element_type=jnp.float32
        )
        probs = []
        for h in range(local_heads):
            span = slice(h * total, (h + 1) * total)
            logits = scores[:, span] * scale + bias[:, span]
            weights = jnp.exp(logits - jnp.max(logits, axis=-1, keepdims=True))
            inverse = 1.0 / jnp.sum(weights, axis=-1, keepdims=True)
            probs.append((weights * inverse).astype(jnp.bfloat16))
        mixed = jnp.dot(
            jnp.concatenate(probs, axis=1), values, preferred_element_type=jnp.float32
        ).astype(jnp.bfloat16)
        attended[s] = mixed.reshape(n_row, token_rows, local_width)

    def give(first, last):
        for j in range(n_row - 1, 0, -1):
            target = nearest(j)
            for s in range(first, last):
                send(
                    attended.at[s, target],
                    heads_in.at[me * samples + s],
                    sent.at[0],
                    att_got.at[me],
                    {"row": target},
                )
        for s in range(first, last):
            heads_in[me * samples + s] = attended[s, me]

    def take_attended(source):
        arrive(heads_in.at[pl.ds(source * samples, samples)], att_got.at[source])

    def build_bias():
        lanes_at = lax.broadcasted_iota(jnp.int32, (part_rows, LANES), 1)
        for tile in range(total // LANES):
            padded = lanes_at[:stripes] + tile * LANES >= valid[0]
            for r in range(n_row):
                parts = [bias_recv[r * n_plane + tile * fold + m] for m in range(fold)]
                for q in range(fold):
                    whole = None
                    for m in range(fold):
                        shift = ((m - q) % fold) * tile_cols
                        turned = pltpu.roll(parts[m], shift, 1) if shift else parts[m]
                        whole = (
                            turned
                            if whole is None
                            else jnp.where(lanes_at >= m * tile_cols, turned, whole)
                        )
                    at = r * tile_rows + q * stripes
                    for h in range(local_heads):
                        bias[
                            at : at + stripes,
                            h * total + tile * LANES : h * total + (tile + 1) * LANES,
                        ] = jnp.where(padded, -1e30, whole[h * stripes : (h + 1) * stripes])

    everything = slice(None)
    with mark("tokload"):
        loads["tok"].wait()
        loads["token_gain"].wait()
    with mark("norm"):
        rows = own[...].reshape(samples * token_rows, width).astype(jnp.float32)
        normed = normalize(rows, token_gain[...]).astype(jnp.bfloat16)
        tok[:, me] = normed.reshape(samples, token_rows, width)
    with mark("barrier"):
        await_greetings(barrier)

    early = min(2, samples)
    for s in range(early):
        send_tokens(s)

    @pl.when(jnp.logical_not(relay))
    def _():
        for s in range(early, samples):
            send_tokens(s)

    with mark("pairload"):
        for name in ("asym", "pair", "rel", "pair_gain", "bias_weight"):
            loads[name].wait()
    first_row, first_col = me * tile_rows, plane * tile_cols
    sub = lax.broadcasted_iota(jnp.int32, (tile_cols, LANES), 0)
    lane = lax.broadcasted_iota(jnp.int32, (tile_cols, LANES), 1)
    with mark("pairprep"):
        col_chain = jnp.zeros((tile_cols, LANES), jnp.int32)
        for j in range(tile_cols):
            col_chain = jnp.where(sub == j, asym[first_col + j], col_chain)
        reach = bins // 2 - 1
        turned_weight = bias_weight[...]
    def pair_stripes(first, last):
        for t in range(first, last):
            hots, rows = [], []
            for q in range(fold):
                i = q * stripes + t
                offset = jnp.clip(first_row + i - first_col - sub, -reach, reach) + reach
                bin_ids = jnp.where(col_chain == asym[first_row + i], offset, bins - 1)
                hots.append(jnp.where(bin_ids == lane, 1.0, 0.0).astype(jnp.bfloat16))
                rows.append(pair[i].astype(jnp.float32))
            summed = jnp.concatenate(rows, axis=0) + jnp.dot(
                jnp.concatenate(hots, axis=0), rel[...], preferred_element_type=jnp.float32
            )
            normed_pair = normalize(summed, pair_gain[...]).astype(jnp.bfloat16)
            projected = lax.dot_general(
                turned_weight, normed_pair, (((1,), (1,)), ((), ())), preferred_element_type=jnp.float32
            )
            bias_send[pl.ds(t, all_heads, stride=stripes), :] = projected

    for r in range(rounds):
        greet(greeting.at[r])
        with mark("pair"):
            pair_stripes(r * stripes // rounds, (r + 1) * stripes // rounds)
        with mark("greeting"):
            await_greetings(greeting.at[r])

    with mark("loads"):
        for name in ("ow", "qkv", "valid"):
            loads[name].wait()
    send_bias()
    own_bias.start()

    @pl.when(relay)
    def _():
        send_ow()
        for s in range(early, samples):
            send_tokens(s)

    @pl.when(edge)
    def _():
        with mark("project"):
            project(me)

    def step(distance):
        for s in range(early if distance == 1 else 0, samples):
            with mark("tokens"):
                take_tokens(s, distance)
            if distance == 1 and s == min(3, samples - 1):

                @pl.when(relay)
                def _():
                    with mark("ow0"):
                        for k in range(1, n_row):
                            spread_ow(k)

        @pl.when(edge)
        def _():
            with mark("project"):
                project(jnp.where(me == 0, distance, me - distance))

    def first_bias():
        with mark("bias0"):
            for k in range(1, n_row):
                pass_bias(k)

    if n_row > 2:
        with mark("tokens0"):
            for s in range(early):
                take_tokens(s, 1)

    @pl.when(relay)
    def _():
        first_bias()

    if n_row > 2:
        step(1)

    @pl.when(jnp.logical_not(relay))
    def _():
        first_bias()

    for distance in range(2, n_row - 1):
        step(distance)

    def relay_ow():
        @pl.when(relay)
        def _():
            with mark("ow1"):
                collect_ow()

    def prepare_bias():
        with mark("bias2"):
            own_bias.wait()
            take_bias()
        with mark("build"):
            build_bias()

    def finish_samples(first, last):
        with mark("attend"):
            for s in range(first, last):
                attend(s)
        with mark("give"):
            give(first, last)

    batch = max(samples // 2, 1)
    batches = [(first, min(first + batch, samples)) for first in range(0, samples, batch)]

    @pl.when(edge)
    def _():
        prepare_bias()
        for first, last in batches:
            with mark("tokense"):
                for s in range(first, last):
                    take_tokens(s, n_row - 1)
            with mark("project"):
                project(n_row - 1 - me, slice(first, last))
            finish_samples(first, last)
            if first == 0:
                relay_ow()

    @pl.when(jnp.logical_not(edge))
    def _():
        for s in range(samples):
            with mark("tokensi"):
                take_tokens(s, n_row - 1)
        with mark("projecti"):
            project(slice(None))
        prepare_bias()
        for first, last in batches:
            finish_samples(first, last)
        relay_ow()

    @pl.when(jnp.logical_not(relay))
    def _():
        with mark("ow3"):
            take_ow()

    def term(source):
        flat = heads_in[pl.ds(source * samples, samples)].reshape(samples * token_rows, local_width)
        return jnp.dot(flat, ow[source], preferred_element_type=jnp.float32)

    with mark("product0"):
        flat_shape = (samples * token_rows, width)
        total_sum[...] = own[...].reshape(flat_shape).astype(jnp.float32) + term(me)
    for j in range(1, n_row):
        source = nearest(j)
        with mark("attwait"):
            take_attended(source)
        with mark("product"):
            if j < n_row - 1:
                total_sum[...] += term(source)
            else:
                result = total_sum[...] + term(source)
                out[...] = result.astype(out.dtype).reshape(samples, token_rows, width)

    with mark("fin"):
        for row in range(n_row):

            @pl.when(me == row)
            def _():
                if row < n_row - 1:
                    awaiting(tok.at[:, pl.ds(0, row + 1)], tok_sent.at[1]).wait_send()
                if row > 0:
                    awaiting(tok.at[:, pl.ds(0, n_row - row)], tok_sent.at[0]).wait_send()

        awaiting(bias_recv.at[pl.ds(0, n_row * n_plane - 1)], sent.at[1]).wait_send()
        awaiting(attended.at[:, pl.ds(0, n_row - 1)], sent.at[0]).wait_send()

        @pl.when(relay)
        def _():
            awaiting(ow.at[pl.ds(0, n_row - 1)], sent.at[2]).wait_send()
            for e in range(1, n_samp):
                awaiting(ow.at[pl.ds(0, n_row - 1)], ow_sent.at[e - 1]).wait_send()


def per_device(
    axes,
    pair_repr,
    asym_id,
    valid_len,
    rel_embed,
    pair_gain,
    bias_weight,
    tokens,
    token_gain,
    qkv_weight,
    out_weight,
):
    n_job, n_row, n_col, n_samp = axes
    samples, token_rows, width = tokens.shape
    total = n_row * token_rows
    n_plane = n_col * n_samp
    heads = bias_weight.shape[1]
    local_heads = heads // n_row
    tile_rows, tile_cols, channels = pair_repr.shape
    local_width = qkv_weight.shape[-1]
    out_rows = out_weight.shape[1]
    cuts = (1 if out_rows % (16 * n_job) else n_job, 1 if width % (LANES * n_col) else n_col)
    stripes = tile_rows // (LANES // tile_cols)
    part_rows = local_heads * stripes
    bf16, f32 = jnp.bfloat16, jnp.float32
    dma = pltpu.SemaphoreType.DMA
    any_spec = pl.BlockSpec(memory_space=pltpu.HBM)
    return pl.pallas_call(
        functools.partial(kernel, axes, cuts),
        out_shape=jax.ShapeDtypeStruct(tokens.shape, tokens.dtype),
        in_specs=[any_spec] * 10,
        out_specs=pl.BlockSpec(memory_space=pltpu.VMEM),
        scratch_shapes=[
            pltpu.SMEM(asym_id.shape, jnp.int32),
            pltpu.SMEM(valid_len.shape, jnp.int32),
            pltpu.VMEM(pair_repr.shape, bf16),
            pltpu.VMEM(rel_embed.shape, bf16),
            pltpu.VMEM((1, channels), f32),
            pltpu.VMEM(bias_weight.shape[::-1], bf16),
            pltpu.VMEM(token_gain.shape, f32),
            pltpu.VMEM((3, local_width, width), bf16),
            pltpu.VMEM(tokens.shape, bf16),
            pltpu.VMEM((samples, n_row, token_rows, width), bf16),
            pltpu.VMEM((n_row, out_rows, width), bf16),
            pltpu.VMEM((heads * stripes, LANES), f32),
            pltpu.VMEM((n_row * n_plane, part_rows, LANES), f32),
            pltpu.VMEM((total, local_heads * total), f32),
            pltpu.VMEM((samples, n_row, token_rows, local_width), bf16),
            pltpu.VMEM((samples, n_row, token_rows, local_width), bf16),
            pltpu.VMEM((samples, n_row, token_rows, local_width), bf16),
            pltpu.VMEM((samples, n_row, token_rows, local_width), bf16),
            pltpu.VMEM((n_row * samples, token_rows, local_width), bf16),
            pltpu.VMEM((samples * token_rows, width), f32),
            dma((11,)),
            dma((samples, n_row)),
            dma((2,)),
            dma((n_row,)),
            dma((n_row + 1,)),
            dma((max(n_samp - 1, 1),)),
            dma((n_row,)),
            dma((3,)),
            pltpu.SemaphoreType.REGULAR((max(n_row - 2, 2),)),
        ],
        compiler_params=pltpu.CompilerParams(
            collective_id=0, has_side_effects=True, vmem_limit_bytes=24 * 1024 * 1024
        ),
    )(
        *(
            operand if operand is valid_len else pltpu.with_memory_space_constraint(operand, pltpu.HBM)
            for operand in (
                asym_id,
                valid_len,
                pair_repr,
                rel_embed,
                pair_gain.reshape(1, channels),
                bias_weight.T,
                tokens,
                token_gain,
                jnp.swapaxes(qkv_weight, 2, 3),
                out_weight,
            )
        )
    )


def solution(mesh):
    axes = tuple(mesh.shape[name] for name in ("job", "row", "col", "samp"))
    return jax.shard_map(
        functools.partial(per_device, axes),
        mesh=mesh,
        in_specs=(
            P(("job", "row"), ("col", "samp"), None),
            P("job"),
            P("job"),
            P(),
            P(),
            P(),
            P(("job", "col", "samp"), "row", None),
            P(),
            P(None, None, None, "row"),
            P(None, "row", None),
        ),
        out_specs=P(("job", "col", "samp"), "row", None),
        check_vma=False,
    )
```

```python
import contextlib
import functools
import math

import jax
import jax.numpy as jnp
from jax import lax
from jax.experimental import pallas as pl
from jax.experimental.pallas import tpu as pltpu
from jax.sharding import PartitionSpec as P

HEAD_DIM = 48
EPSILON = 1e-05
LANES = 128
MESH = pl.DeviceIdType.MESH
mark = contextlib.nullcontext


def normalize(values, gain_vector):
    average = jnp.mean(values, axis=-1, keepdims=True)
    centered = values - average
    variance = jnp.mean(centered * centered, axis=-1, keepdims=True)
    return centered * lax.rsqrt(variance + EPSILON) * gain_vector


def back(position, shift, size):
    return lax.rem(position + (size - shift), size) if shift else position


def aligned(value, unit):
    return value if isinstance(value, int) else pl.multiple_of(value, unit)


def kernel(
    axes,
    cuts,
    asym_hbm,
    valid_hbm,
    pair_hbm,
    rel_hbm,
    pair_gain_hbm,
    bias_weight_hbm,
    tokens_hbm,
    token_gain_hbm,
    qkv_hbm,
    out_weight_hbm,
    out,
    asym,
    valid,
    pair,
    rel,
    pair_gain,
    bias_weight,
    token_gain,
    qkv,
    own,
    tok,
    ow,
    bias_send,
    bias_recv,
    bias,
    query,
    key,
    value,
    attended,
    heads_in,
    total_sum,
    local_sem,
    tok_got,
    tok_sent,
    bias_got,
    ow_got,
    ow_sent,
    att_got,
    sent,
    greeting,
):
    n_job, n_row, n_col, n_samp = axes
    job, me = lax.axis_index("job"), lax.axis_index("row")
    col, samp = lax.axis_index("col"), lax.axis_index("samp")
    samples, token_rows, width = tokens_hbm.shape
    total = n_row * token_rows
    tile_rows, tile_cols, channels = pair.shape
    bins = rel.shape[0]
    plane = col * n_samp + samp
    all_heads = bias_weight.shape[0]
    local_heads = all_heads // n_row
    local_width = local_heads * HEAD_DIM
    fold = LANES // tile_cols
    stripes = tile_rows // fold
    part_rows = bias_recv.shape[1]
    out_rows = ow.shape[1]
    n_plane = n_col * n_samp
    p_job, p_col = cuts
    pieces = p_job * p_col
    piece_rows, piece_cols = out_rows // p_job, width // p_col
    relay = samp == n_samp - 1

    def row_peer(k):
        return lax.rem(me + k, n_row)

    def row_source(k):
        return back(me, k, n_row)

    def send(source, target, left, got, device):
        pltpu.make_async_remote_copy(
            src_ref=source,
            dst_ref=target,
            send_sem=left,
            recv_sem=got,
            device_id=device,
            device_id_type=MESH,
        ).start()

    def awaiting(ref, semaphore):
        return pltpu.make_async_remote_copy(
            src_ref=ref,
            dst_ref=ref,
            send_sem=semaphore,
            recv_sem=semaphore,
            device_id={"row": row_peer(1)},
            device_id_type=MESH,
        )

    def arrive(ref, semaphore):
        awaiting(ref, semaphore).wait_recv()

    has_right, has_left = me < n_row - 1, me > 0
    edge = jnp.logical_or(me == 0, me == n_row - 1)

    def greet(semaphore):
        for name, spot, size in (("col", col, n_col), ("samp", samp, n_samp), ("job", job, p_job)):
            for k in range(1, size):
                device = {name: lax.rem(spot + k, size)}
                pl.semaphore_signal(semaphore, inc=1, device_id=device, device_id_type=MESH)

        @pl.when(has_right)
        def _():
            device = {"row": jnp.minimum(me + 1, n_row - 1)}
            pl.semaphore_signal(semaphore, inc=1, device_id=device, device_id_type=MESH)

        @pl.when(has_left)
        def _():
            device = {"row": jnp.maximum(me - 1, 0)}
            pl.semaphore_signal(semaphore, inc=1, device_id=device, device_id_type=MESH)

    def await_greetings(semaphore):
        others = (n_col - 1) + (n_samp - 1) + (p_job - 1)
        pl.semaphore_wait(semaphore, others + jnp.where(edge, 1, 2))

    rounds = greeting.shape[0]
    barrier = pltpu.get_barrier_semaphore()
    greet(barrier)

    loads = {}
    for index, (name, source, target) in enumerate(
        (
            ("asym", asym_hbm, asym),
            ("pair", pair_hbm, pair),
            ("rel", rel_hbm, rel),
            ("pair_gain", pair_gain_hbm, pair_gain),
            ("bias_weight", bias_weight_hbm, bias_weight),
            ("qkv", qkv_hbm.at[0], qkv),
            ("token_gain", token_gain_hbm, token_gain),
            ("ow", out_weight_hbm.at[0], ow.at[me]),
            ("valid", valid_hbm, valid),
        )
    ):
        loads[name] = pltpu.make_async_copy(source, target, local_sem.at[index])
    loads["tok"] = pltpu.make_async_copy(tokens_hbm, own, local_sem.at[9])
    for name in ("tok", "token_gain", "asym", "pair", "rel", "pair_gain", "bias_weight", "qkv", "ow", "valid"):
        loads[name].start()

    def ow_piece(source, a, b):
        first = aligned(lax.rem(job + a, n_job) * piece_rows if p_job > 1 else 0, piece_rows)
        start = aligned(lax.rem(col + b, n_col) * piece_cols if p_col > 1 else 0, piece_cols)
        return ow.at[source, pl.ds(first, piece_rows), pl.ds(start, piece_cols)]

    chips = [(a, b) for a in range(p_job) for b in range(p_col)]

    def send_ow():
        for k in range(n_row - 1, 0, -1):
            send(ow_piece(me, 0, 0), ow_piece(me, 0, 0), sent.at[2], ow_got.at[k - 1], {"row": row_peer(k)})

    def pair_ow(k, a, b):
        piece = ow_piece(row_source(k), a, b)
        for e in range(1, n_samp):
            device = {"samp": lax.rem(samp + e, n_samp)}
            send(piece, piece, ow_sent.at[e - 1], ow_got.at[n_row], device)

    def spread_ow(k):
        piece = ow_piece(row_source(k), 0, 0)
        arrive(piece, ow_got.at[k - 1])
        for a, b in chips[1:]:
            device = {
                name: lax.rem(spot + step, size)
                for name, spot, step, size in (("job", job, a, n_job), ("col", col, b, n_col))
                if step
            }
            send(piece, piece, sent.at[2], ow_got.at[n_row - 1], device)
        pair_ow(k, 0, 0)

    def collect_ow():
        if pieces > 1:
            others = ow.at[pl.ds(0, n_row - 1), pl.ds(0, out_rows - out_rows // pieces)]
            arrive(others, ow_got.at[n_row - 1])
            for k in range(1, n_row):
                for a, b in chips[1:]:
                    pair_ow(k, a, b)

    def take_ow():
        arrive(ow.at[pl.ds(0, n_row - 1)], ow_got.at[n_row])

    low = 2 * me < n_row
    outward = jnp.where(low, -1, 1)
    near = jnp.minimum(me, n_row - 1 - me)

    def nearest(j):
        step = (j + 1) // 2
        both = jnp.where(low == (j % 2 == 1), -step, step)
        one = jnp.where(low, j - near, near - j)
        return me + jnp.where(j <= 2 * near, both, one)

    def push_tokens(s, source, way):
        target = me + way

        @pl.when(jnp.logical_and(target >= 0, target < n_row))
        def _():
            send(
                tok.at[s, source],
                tok.at[s, source],
                tok_sent.at[(way + 1) // 2],
                tok_got.at[s, source],
                {"row": jnp.clip(target, 0, n_row - 1)},
            )

    def send_tokens(s):
        push_tokens(s, me, -outward)
        push_tokens(s, me, outward)

    def take_tokens(s, distance):
        for way in (outward, -outward):
            source = me + way * distance

            @pl.when(jnp.logical_and(source >= 0, source < n_row))
            def _():
                place = jnp.clip(source, 0, n_row - 1)
                arrive(tok.at[s, place], tok_got.at[s, place])
                push_tokens(s, place, -way)

    def bias_part(target):
        return bias_send.at[
            pl.ds(pl.multiple_of(target * part_rows, part_rows), part_rows)
        ]

    def spread_bias(k):
        place = bias_recv.at[row_source(k) * n_plane + plane]
        held = place if k else bias_part(me)
        for m in range(1, n_plane):
            other = lax.rem(plane + m, n_plane)
            send(
                held,
                place,
                sent.at[1],
                bias_got.at[n_row - 1],
                {"col": lax.div(other, n_samp), "samp": lax.rem(other, n_samp)},
            )

    def send_bias():
        for k in range(n_row - 1, 0, -1):
            target = row_peer(k)
            send(
                bias_part(target),
                bias_recv.at[me * n_plane + plane],
                sent.at[1],
                bias_got.at[k - 1],
                {"row": target},
            )
        spread_bias(0)

    def pass_bias(k):
        arrive(bias_recv.at[row_source(k) * n_plane + plane], bias_got.at[k - 1])
        spread_bias(k)

    def take_bias():
        if n_plane > 1:
            arrive(bias_recv.at[pl.ds(0, n_row * (n_plane - 1))], bias_got.at[n_row - 1])

    own_bias = pltpu.make_async_copy(
        bias_part(me), bias_recv.at[me * n_plane + plane], local_sem.at[10]
    )

    head_of_lane = lax.broadcasted_iota(jnp.int32, (total, local_width), 1)
    head_masks = [
        jnp.logical_and(head_of_lane >= h * HEAD_DIM, head_of_lane < (h + 1) * HEAD_DIM)
        for h in range(local_heads)
    ]
    scale = 1.0 / math.sqrt(HEAD_DIM)

    def project(sources, chosen=slice(None)):
        normed = tok[chosen, sources].reshape(-1, width)
        for index, target in enumerate((query, key, value)):
            done = lax.dot_general(
                normed, qkv[index], (((1,), (1,)), ((), ())), preferred_element_type=jnp.float32
            ).astype(jnp.bfloat16)
            target[chosen, sources] = done.reshape(target[chosen, sources].shape)

    def attend(s):
        whole = (total, local_width)
        keys = key[s].reshape(whole).astype(jnp.float32)
        values = value[s].reshape(whole).astype(jnp.float32)
        keys = jnp.concatenate(
            [jnp.where(mask, keys, 0.0).astype(jnp.bfloat16) for mask in head_masks], axis=0
        )
        values = jnp.concatenate(
            [jnp.where(mask, values, 0.0).astype(jnp.bfloat16) for mask in head_masks], axis=0
        )
        scores = lax.dot_general(
            query[s].reshape(whole), keys, (((1,), (1,)), ((), ())), preferred_element_type=jnp.float32
        )
        probs = []
        for h in range(local_heads):
            span = slice(h * total, (h + 1) * total)
            logits = scores[:, span] * scale + bias[:, span]
            weights = jnp.exp(logits - jnp.max(logits, axis=-1, keepdims=True))
            inverse = 1.0 / jnp.sum(weights, axis=-1, keepdims=True)
            probs.append((weights * inverse).astype(jnp.bfloat16))
        mixed = jnp.dot(
            jnp.concatenate(probs, axis=1), values, preferred_element_type=jnp.float32
        ).astype(jnp.bfloat16)
        attended[s] = mixed.reshape(n_row, token_rows, local_width)

    def give(first, last):
        for j in range(n_row - 1, 0, -1):
            target = nearest(j)
            for s in range(first, last):
                send(
                    attended.at[s, target],
                    heads_in.at[me * samples + s],
                    sent.at[0],
                    att_got.at[me],
                    {"row": target},
                )
        for s in range(first, last):
            heads_in[me * samples + s] = attended[s, me]

    def take_attended(source):
        arrive(heads_in.at[pl.ds(source * samples, samples)], att_got.at[source])

    def build_bias():
        lanes_at = lax.broadcasted_iota(jnp.int32, (part_rows, LANES), 1)
        for tile in range(total // LANES):
            padded = lanes_at[:stripes] + tile * LANES >= valid[0]
            for r in range(n_row):
                parts = [bias_recv[r * n_plane + tile * fold + m] for m in range(fold)]
                for q in range(fold):
                    whole = None
                    for m in range(fold):
                        shift = ((m - q) % fold) * tile_cols
                        turned = pltpu.roll(parts[m], shift, 1) if shift else parts[m]
                        whole = (
                            turned
                            if whole is None
                            else jnp.where(lanes_at >= m * tile_cols, turned, whole)
                        )
                    at = r * tile_rows + q * stripes
                    for h in range(local_heads):
                        bias[
                            at : at + stripes,
                            h * total + tile * LANES : h * total + (tile + 1) * LANES,
                        ] = jnp.where(padded, -1e30, whole[h * stripes : (h + 1) * stripes])

    everything = slice(None)
    with mark("tokload"):
        loads["tok"].wait()
        loads["token_gain"].wait()
    with mark("norm"):
        rows = own[...].reshape(samples * token_rows, width).astype(jnp.float32)
        normed = normalize(rows, token_gain[...]).astype(jnp.bfloat16)
        tok[:, me] = normed.reshape(samples, token_rows, width)
    with mark("barrier"):
        await_greetings(barrier)

    early = min(2, samples)
    for s in range(early):
        send_tokens(s)

    @pl.when(jnp.logical_not(relay))
    def _():
        for s in range(early, samples):
            send_tokens(s)

    with mark("pairload"):
        for name in ("asym", "pair", "rel", "pair_gain", "bias_weight"):
            loads[name].wait()
    first_row, first_col = me * tile_rows, plane * tile_cols
    sub = lax.broadcasted_iota(jnp.int32, (tile_cols, LANES), 0)
    lane = lax.broadcasted_iota(jnp.int32, (tile_cols, LANES), 1)
    with mark("pairprep"):
        col_chain = jnp.zeros((tile_cols, LANES), jnp.int32)
        for j in range(tile_cols):
            col_chain = jnp.where(sub == j, asym[first_col + j], col_chain)
        reach = bins // 2 - 1
        turned_weight = bias_weight[...]
    def pair_stripes(first, last):
        for t in range(first, last):
            hots, rows = [], []
            for q in range(fold):
                i = q * stripes + t
                offset = jnp.clip(first_row + i - first_col - sub, -reach, reach) + reach
                bin_ids = jnp.where(col_chain == asym[first_row + i], offset, bins - 1)
                hots.append(jnp.where(bin_ids == lane, 1.0, 0.0).astype(jnp.bfloat16))
                rows.append(pair[i].astype(jnp.float32))
            summed = jnp.concatenate(rows, axis=0) + jnp.dot(
                jnp.concatenate(hots, axis=0), rel[...], preferred_element_type=jnp.float32
            )
            normed_pair = normalize(summed, pair_gain[...]).astype(jnp.bfloat16)
            projected = lax.dot_general(
                turned_weight, normed_pair, (((1,), (1,)), ((), ())), preferred_element_type=jnp.float32
            )
            bias_send[pl.ds(t, all_heads, stride=stripes), :] = projected

    for r in range(rounds):
        greet(greeting.at[r])
        with mark("pair"):
            pair_stripes(r * stripes // rounds, (r + 1) * stripes // rounds)
        with mark("greeting"):
            await_greetings(greeting.at[r])

    with mark("loads"):
        for name in ("ow", "qkv", "valid"):
            loads[name].wait()
    send_bias()
    own_bias.start()

    @pl.when(relay)
    def _():
        send_ow()
        for s in range(early, samples):
            send_tokens(s)

    @pl.when(edge)
    def _():
        with mark("project"):
            project(me)

    def step(distance):
        for s in range(early if distance == 1 else 0, samples):
            with mark("tokens"):
                take_tokens(s, distance)
            if distance == 1 and s == min(3, samples - 1):

                @pl.when(relay)
                def _():
                    with mark("ow0"):
                        for k in range(1, n_row):
                            spread_ow(k)

        @pl.when(edge)
        def _():
            with mark("project"):
                project(jnp.where(me == 0, distance, me - distance))

    def first_bias():
        with mark("bias0"):
            for k in range(1, n_row):
                pass_bias(k)

    if n_row > 2:
        with mark("tokens0"):
            for s in range(early):
                take_tokens(s, 1)

    @pl.when(relay)
    def _():
        first_bias()

    if n_row > 2:
        step(1)

    @pl.when(jnp.logical_not(relay))
    def _():
        first_bias()

    for distance in range(2, n_row - 1):
        step(distance)

    def relay_ow():
        @pl.when(relay)
        def _():
            with mark("ow1"):
                collect_ow()

    def prepare_bias():
        with mark("bias2"):
            own_bias.wait()
            take_bias()
        with mark("build"):
            build_bias()

    def finish_samples(first, last):
        with mark("attend"):
            for s in range(first, last):
                attend(s)
        with mark("give"):
            give(first, last)

    batch = max(samples // 2, 1)
    batches = [(first, min(first + batch, samples)) for first in range(0, samples, batch)]

    @pl.when(edge)
    def _():
        prepare_bias()
        for first, last in batches:
            with mark("tokense"):
                for s in range(first, last):
                    take_tokens(s, n_row - 1)
            with mark("project"):
                project(n_row - 1 - me, slice(first, last))
            finish_samples(first, last)
            if first == 0:
                relay_ow()

    @pl.when(jnp.logical_not(edge))
    def _():
        for s in range(samples):
            with mark("tokensi"):
                take_tokens(s, n_row - 1)
        with mark("projecti"):
            project(slice(None))
        prepare_bias()
        for first, last in batches:
            finish_samples(first, last)
        relay_ow()

    @pl.when(jnp.logical_not(relay))
    def _():
        with mark("ow3"):
            take_ow()

    def term(source):
        flat = heads_in[pl.ds(source * samples, samples)].reshape(samples * token_rows, local_width)
        return jnp.dot(flat, ow[source], preferred_element_type=jnp.float32)

    with mark("product0"):
        flat_shape = (samples * token_rows, width)
        total_sum[...] = own[...].reshape(flat_shape).astype(jnp.float32) + term(me)
    for j in range(1, n_row):
        source = nearest(j)
        with mark("attwait"):
            take_attended(source)
        with mark("product"):
            if j < n_row - 1:
                total_sum[...] += term(source)
            else:
                result = total_sum[...] + term(source)
                out[...] = result.astype(out.dtype).reshape(samples, token_rows, width)

    with mark("fin"):
        for row in range(n_row):

            @pl.when(me == row)
            def _():
                if row < n_row - 1:
                    awaiting(tok.at[:, pl.ds(0, row + 1)], tok_sent.at[1]).wait_send()
                if row > 0:
                    awaiting(tok.at[:, pl.ds(0, n_row - row)], tok_sent.at[0]).wait_send()

        awaiting(bias_recv.at[pl.ds(0, n_row * n_plane - 1)], sent.at[1]).wait_send()
        awaiting(attended.at[:, pl.ds(0, n_row - 1)], sent.at[0]).wait_send()

        @pl.when(relay)
        def _():
            awaiting(ow.at[pl.ds(0, n_row - 1)], sent.at[2]).wait_send()
            for e in range(1, n_samp):
                awaiting(ow.at[pl.ds(0, n_row - 1)], ow_sent.at[e - 1]).wait_send()


def per_device(
    axes,
    pair_repr,
    asym_id,
    valid_len,
    rel_embed,
    pair_gain,
    bias_weight,
    tokens,
    token_gain,
    qkv_weight,
    out_weight,
):
    n_job, n_row, n_col, n_samp = axes
    samples, token_rows, width = tokens.shape
    total = n_row * token_rows
    n_plane = n_col * n_samp
    heads = bias_weight.shape[1]
    local_heads = heads // n_row
    tile_rows, tile_cols, channels = pair_repr.shape
    local_width = qkv_weight.shape[-1]
    out_rows = out_weight.shape[1]
    cuts = (1 if out_rows % (16 * n_job) else n_job, 1 if width % (LANES * n_col) else n_col)
    stripes = tile_rows // (LANES // tile_cols)
    part_rows = local_heads * stripes
    bf16, f32 = jnp.bfloat16, jnp.float32
    dma = pltpu.SemaphoreType.DMA
    any_spec = pl.BlockSpec(memory_space=pltpu.HBM)
    return pl.pallas_call(
        functools.partial(kernel, axes, cuts),
        out_shape=jax.ShapeDtypeStruct(tokens.shape, tokens.dtype),
        in_specs=[any_spec] * 10,
        out_specs=pl.BlockSpec(memory_space=pltpu.VMEM),
        scratch_shapes=[
            pltpu.SMEM(asym_id.shape, jnp.int32),
            pltpu.SMEM(valid_len.shape, jnp.int32),
            pltpu.VMEM(pair_repr.shape, bf16),
            pltpu.VMEM(rel_embed.shape, bf16),
            pltpu.VMEM((1, channels), f32),
            pltpu.VMEM(bias_weight.shape[::-1], bf16),
            pltpu.VMEM(token_gain.shape, f32),
            pltpu.VMEM((3, local_width, width), bf16),
            pltpu.VMEM(tokens.shape, bf16),
            pltpu.VMEM((samples, n_row, token_rows, width), bf16),
            pltpu.VMEM((n_row, out_rows, width), bf16),
            pltpu.VMEM((heads * stripes, LANES), f32),
            pltpu.VMEM((n_row * n_plane, part_rows, LANES), f32),
            pltpu.VMEM((total, local_heads * total), f32),
            pltpu.VMEM((samples, n_row, token_rows, local_width), bf16),
            pltpu.VMEM((samples, n_row, token_rows, local_width), bf16),
            pltpu.VMEM((samples, n_row, token_rows, local_width), bf16),
            pltpu.VMEM((samples, n_row, token_rows, local_width), bf16),
            pltpu.VMEM((n_row * samples, token_rows, local_width), bf16),
            pltpu.VMEM((samples * token_rows, width), f32),
            dma((11,)),
            dma((samples, n_row)),
            dma((2,)),
            dma((n_row,)),
            dma((n_row + 1,)),
            dma((max(n_samp - 1, 1),)),
            dma((n_row,)),
            dma((3,)),
            pltpu.SemaphoreType.REGULAR((max(n_row - 2, 2),)),
        ],
        compiler_params=pltpu.CompilerParams(
            collective_id=0, has_side_effects=True, vmem_limit_bytes=24 * 1024 * 1024
        ),
    )(
        *(
            operand if operand is valid_len else pltpu.with_memory_space_constraint(operand, pltpu.HBM)
            for operand in (
                asym_id,
                valid_len,
                pair_repr,
                rel_embed,
                pair_gain.reshape(1, channels),
                bias_weight.T,
                tokens,
                token_gain,
                jnp.swapaxes(qkv_weight, 2, 3),
                out_weight,
            )
        )
    )


def solution(mesh):
    axes = tuple(mesh.shape[name] for name in ("job", "row", "col", "samp"))
    return jax.shard_map(
        functools.partial(per_device, axes),
        mesh=mesh,
        in_specs=(
            P(("job", "row"), ("col", "samp"), None),
            P("job"),
            P("job"),
            P(),
            P(),
            P(),
            P(("job", "col", "samp"), "row", None),
            P(),
            P(None, None, None, "row"),
            P(None, "row", None),
        ),
        out_specs=P(("job", "col", "samp"), "row", None),
        check_vma=False,
    )
```
